32 devices in a mesh: clip: 16 (over z, x, core), seq: 2 (over y).
Axes of the slice: x: 2, y: 2, z: 4, core: 2. Of those that a mesh axis runs over, the one named last changes fastest.
Arguments:
- frames: bfloat16 [16, 1500, 768], P('clip', 'seq'), may hold values from -6 to 6
- norm1_gain: bfloat16 [768], P(('clip', 'seq')), may hold values from 0.5 to 1.5
- norm1_shift: bfloat16 [768], P(('clip', 'seq')), may hold values from -3 to 3
- query_weight: bfloat16 [768, 768], P(('clip', 'seq')), may hold values from -0.21875 to 0.21875
- query_bias: bfloat16 [768], P(('clip', 'seq')), may hold values from -3 to 3
- key_weight: bfloat16 [768, 768], P(('clip', 'seq')), may hold values from -0.21875 to 0.21875
- value_weight: bfloat16 [768, 768], P(('clip', 'seq')), may hold values from -0.21875 to 0.21875
- value_bias: bfloat16 [768], P(('clip', 'seq')), may hold values from -3 to 3
- out_weight: bfloat16 [768, 768], P(('clip', 'seq')), may hold values from -6 to 6
- out_bias: bfloat16 [768], P(('clip', 'seq')), may hold values from -3 to 3
- norm2_gain: bfloat16 [768], P(('clip', 'seq')), may hold values from 0.5 to 1.5
- norm2_shift: bfloat16 [768], P(('clip', 'seq')), may hold values from -3 to 3
- hidden_weight: bfloat16 [768, 3072], P(('clip', 'seq')), may hold values from -0.21875 to 0.21875
- hidden_bias: bfloat16 [3072], P(('clip', 'seq')), may hold values from -3 to 3
- output_weight: bfloat16 [3072, 768], P(('clip', 'seq')), may hold values from -0.109375 to 0.109375
- output_bias: bfloat16 [768], P(('clip', 'seq')), may hold values from -3 to 3
- out_grad: bfloat16 [16, 1500, 768], P('clip', 'seq'), may hold values from -6 to 6
Outputs:
- encoded: bfloat16 [16, 1500, 768], P('clip', 'seq')
- frames_grad: bfloat16 [16, 1500, 768], P('clip', 'seq')
- norm1_gain_grad: float32 [768], P(('clip', 'seq'))
- norm1_shift_grad: float32 [768], P(('clip', 'seq'))
- query_weight_grad: float32 [768, 768], P(('clip', 'seq'))
- query_bias_grad: float32 [768], P(('clip', 'seq'))
- key_weight_grad: float32 [768, 768], P(('clip', 'seq'))
- value_weight_grad: float32 [768, 768], P(('clip', 'seq'))
- value_bias_grad: float32 [768], P(('clip', 'seq'))
- out_weight_grad: float32 [768, 768], P(('clip', 'seq'))
- out_bias_grad: float32 [768], P(('clip', 'seq'))
- norm2_gain_grad: float32 [768], P(('clip', 'seq'))
- norm2_shift_grad: float32 [768], P(('clip', 'seq'))
- hidden_weight_grad: float32 [768, 3072], P(('clip', 'seq'))
- hidden_bias_grad: float32 [3072], P(('clip', 'seq'))
- output_weight_grad: float32 [3072, 768], P(('clip', 'seq'))
- output_bias_grad: float32 [768], P(('clip', 'seq'))
The draws below stay inside these ranges and needn't reach their ends.
All inputs are finite; a program needn't handle non-finite values.
Results may differ from the reference program's by a relative error of at most 0.012.
Values may be sent and summed in bfloat16 or wider, within the bound.
A program may use at most 256 MiB of HBM per device.

```python
import jax
import jax.numpy as jnp
from jax import lax

D = 768
H = 12
HD = 64
FF = 3072
FRAMES = 1500
CLIPS = 16


def with_spikes(entries, rng, source, target, parts, factor):
    def block_of(axis_at):
        return (jnp.arange(entries.shape[axis_at]) // (entries.shape[axis_at] // parts)).reshape((-1,) + (1,) * (entries.ndim - 1 - axis_at))

    one_side = jax.random.permutation(rng, parts)[block_of(target)]
    second = (block_of(target) + parts // 2) % parts
    return jnp.where((block_of(source) == one_side) | (block_of(source) == second), factor * entries, entries)


def block_levels(own_key, shape, shards, smallest, high):
    level = 1.0
    for dim, shards_of in shards:
        draws = jax.random.uniform(jax.random.fold_in(jax.random.fold_in(own_key, 6), dim), (shards_of,), jnp.float32, smallest / len(shards), high / len(shards))
        level = level * jnp.repeat(jnp.exp(draws), shape[dim] // shards_of).reshape((-1,) + (1,) * (len(shape) - 1 - dim))
    return level


def centred(rng, shape, scale, bound, pieces=(), held_as=jnp.bfloat16):
    gain = block_levels(rng, shape, pieces, -0.22, 0.18) if pieces else 1.0
    values = jax.random.normal(rng, shape, jnp.float32) * scale * gain
    return jnp.minimum(jnp.maximum(values, -bound), bound).astype(held_as)


def gaussian_with(stream_key, dims, scale, most, pieces, heavy, dtype=jnp.bfloat16):
    drawn = scale * jax.random.normal(stream_key, dims, jnp.float32)
    if pieces:
        drawn = drawn * block_levels(stream_key, dims, pieces, -0.22, 0.18)
    return jnp.clip(with_spikes(drawn, jax.random.fold_in(stream_key, 3), *heavy), -most, most).astype(dtype)


def setup_inputs(seed: int = 0) -> dict:
    keys = jax.random.split(jax.random.key(seed), 18)
    frames = centred(keys[0], (CLIPS, FRAMES, D), 1.0, 6.0, ((0, 16), (1, 2)))
    norm1_gain = jnp.clip(1.0 + 0.1 * jax.random.normal(keys[1], (D,), jnp.float32), 0.5, 1.5).astype(jnp.bfloat16)
    norm1_shift = centred(keys[2], (D,), 0.5, 3.0, ((0, 32),))
    query_weight = centred(keys[3], (D, D), D ** -0.5, 0.21875, ((0, 32),))
    query_bias = centred(keys[4], (D,), 0.5, 3.0, ((0, 32),))
    key_weight = centred(keys[5], (D, D), D ** -0.5, 0.21875, ((0, 32),))
    value_weight = centred(keys[6], (D, D), D ** -0.5, 0.21875, ((0, 32),))
    value_bias = centred(keys[7], (D,), 0.5, 3.0, ((0, 32),))
    out_weight = centred(keys[8], (D, D), 1.0, 6.0, ((0, 32),))
    out_bias = centred(keys[9], (D,), 0.5, 3.0, ((0, 32),))
    norm2_gain = jnp.clip(1.0 + 0.1 * jax.random.normal(keys[10], (D,), jnp.float32), 0.5, 1.5).astype(jnp.bfloat16)
    norm2_shift = centred(keys[11], (D,), 0.5, 3.0, ((0, 32),))
    hidden_weight = centred(keys[12], (D, FF), D ** -0.5, 0.21875, ((0, 32),))
    hidden_bias = centred(keys[13], (FF,), 0.5, 3.0, ((0, 32),))
    output_weight = centred(keys[14], (FF, D), FF ** -0.5, 0.109375, ((0, 32),))
    output_bias = centred(keys[15], (D,), 0.5, 3.0, ((0, 32),))
    out_grad = gaussian_with(keys[16], (CLIPS, FRAMES, D), 1.0, 6.0, ((0, 16), (1, 2)), (0, 2, 16, 2.0))
    return dict(frames=frames, norm1_gain=norm1_gain, norm1_shift=norm1_shift, query_weight=query_weight, query_bias=query_bias, key_weight=key_weight, value_weight=value_weight, value_bias=value_bias, out_weight=out_weight, out_bias=out_bias, norm2_gain=norm2_gain, norm2_shift=norm2_shift, hidden_weight=hidden_weight, hidden_bias=hidden_bias, output_weight=output_weight, output_bias=output_bias, out_grad=out_grad)


epsilon = 1e-05
highest = lax.Precision.HIGHEST

@jax.custom_vjp
def low(v):
    return lax.optimization_barrier(v.astype(jnp.bfloat16)).astype(jnp.float32)

@jax.custom_vjp
def low_back(v):
    return v

def low_keep(v):
    return (low(v), None)

def low_pass(kept, grad):
    return (grad,)

def back_keep(v):
    return (v, None)

def back_low(kept, grad):
    return (low(grad),)
low.defvjp(low_keep, low_pass)
low_back.defvjp(back_keep, back_low)

def both_round(value_in):
    return low_back(low(value_in))

def matmul(left, right):
    return jnp.dot(left, right, precision=highest, preferred_element_type=jnp.float32)

def layer_norm(rows_in, gain_vec, shift_vec):
    center = rows_in - lax.optimization_barrier(jnp.mean(rows_in, axis=-1, keepdims=True))
    spread = lax.optimization_barrier(jnp.mean(center * center, axis=-1, keepdims=True))
    return center * lax.rsqrt(spread + epsilon) * gain_vec + shift_vec

def gelu_exact(rows_in):
    return 0.5 * rows_in * (1.0 + lax.erf(rows_in * 0.7071067811865476))

def heads_first(rows_in):
    return rows_in.reshape(rows_in.shape[0], H, HD).transpose(1, 0, 2)

def encode_clip(params, clip_rows):
    gain_one, shift_one, w_query, b_query, w_key, w_value, b_value, w_out, b_out, gain_two, shift_two, w_hidden, b_hidden, w_output, b_output = params
    normed = low(layer_norm(clip_rows, gain_one, shift_one))
    query_rows = both_round(matmul(normed, w_query) + b_query)
    key_rows = both_round(matmul(normed, w_key))
    value_rows = both_round(matmul(normed, w_value) + b_value)
    scores = low_back(jnp.einsum('hqd,hkd->hqk', heads_first(query_rows), heads_first(key_rows), precision=highest) * HD ** (-0.5))
    row_max = lax.optimization_barrier(jnp.max(scores, axis=-1, keepdims=True))
    exp_scores = jnp.exp(scores - row_max)
    soft_probs = exp_scores / lax.optimization_barrier(jnp.sum(exp_scores, axis=-1, keepdims=True))
    attended = jnp.einsum('hqk,hkd->hqd', low(soft_probs), heads_first(value_rows), precision=highest)
    attended = both_round(attended.transpose(1, 0, 2).reshape(clip_rows.shape[0], D))
    branch = low_back(matmul(attended, w_out) + b_out)
    hidden_in = clip_rows + branch
    normed_two = low(layer_norm(hidden_in, gain_two, shift_two))
    pre_act = low_back(matmul(normed_two, w_hidden) + b_hidden)
    acted = low(gelu_exact(pre_act))
    ff_out = low_back(matmul(acted, w_output) + b_output)
    return hidden_in + ff_out

def reference(frames, norm1_gain, norm1_shift, query_weight, query_bias, key_weight, value_weight, value_bias, out_weight, out_bias, norm2_gain, norm2_shift, hidden_weight, hidden_bias, output_weight, output_bias, out_grad):
    params = tuple((param_in.astype(jnp.float32) for param_in in (norm1_gain, norm1_shift, query_weight, query_bias, key_weight, value_weight, value_bias, out_weight, out_bias, norm2_gain, norm2_shift, hidden_weight, hidden_bias, output_weight, output_bias)))
    inputs = frames.astype(jnp.float32)

    def forward(weights_all, clips_all):

        def one_clip(clip_rows):
            return encode_clip(weights_all, clip_rows)
        return lax.map(jax.checkpoint(one_clip), clips_all)
    output, pull_back = jax.vjp(forward, params, inputs)
    weight_grads, input_grad = pull_back(out_grad.astype(jnp.float32))
    g_gain_one, g_shift_one, g_w_query, g_b_query, g_w_key, g_w_value, g_b_value, g_w_out, g_b_out, g_gain_two, g_shift_two, g_w_hidden, g_b_hidden, g_w_output, g_b_output = weight_grads
    return (output.astype(jnp.bfloat16), input_grad.astype(jnp.bfloat16), g_gain_one, g_shift_one, g_w_query, g_b_query, g_w_key, g_w_value, g_b_value, g_w_out, g_b_out, g_gain_two, g_shift_two, g_w_hidden, g_b_hidden, g_w_output, g_b_output)
```

```python
import functools

import jax
import jax.numpy as jnp
from jax import lax
from jax.experimental import pallas as pl
from jax.experimental.pallas import tpu as pltpu
from jax.sharding import PartitionSpec as P

bf, f32 = jnp.bfloat16, jnp.float32
NEG = -1e30

def nt(a, b):
    return lax.dot_general(a, b, (((1,), (1,)), ((), ())), preferred_element_type=f32)
def nn(a, b):
    return lax.dot_general(a, b, (((1,), (0,)), ((), ())), preferred_element_type=f32)
def tn(a, b):
    return lax.dot_general(a, b, (((0,), (0,)), ((), ())), preferred_element_type=f32)

def lanes(shape):
    return lax.broadcasted_iota(jnp.int32, shape, 1)
def rows(shape):
    return lax.broadcasted_iota(jnp.int32, shape, 0)

def split3(x):
    hi = x.astype(bf); r = x - hi.astype(f32)
    mid = r.astype(bf); lo = (r - mid.astype(f32)).astype(bf)
    return hi.astype(f32), mid.astype(f32), lo.astype(f32)

def fwd_kernel(half, valid, tq, q_ref, k_ref, v_ref, o_ref, wide_ref, l_ref, kc, vc):
    n = k_ref.shape[0]
    @pl.when(pl.program_id(1) == 0)
    def _():
        ln = lanes((n, 128)); pad = lax.rem(rows((n, 128)), half) >= valid
        k = k_ref[...]
        ext = jnp.where((ln == 0) & pad, NEG, 0.0).astype(bf)
        zero = jnp.zeros_like(k)
        kc[0, :, :128] = jnp.where(ln < 64, k, zero)
        kc[1, :, :128] = jnp.where(ln < 64, zero, k)
        kc[0, :, 128:] = ext
        kc[1, :, 128:] = ext
        vc[:, :128] = v_ref[...]
        vc[:, 128:] = jnp.ones((n, 128), bf)
    ln = lanes((tq, 128))
    one = jnp.where(ln == 0, 1.0, 0.0).astype(bf)
    qc = jnp.concatenate([q_ref[...] * jnp.asarray(0.125, bf), one], axis=1)
    outs = []
    for h in range(2):
        s = nt(qc, kc[h])
        m = jnp.max(s, axis=1, keepdims=True)
        p = jnp.exp(s - m).astype(bf)
        o = nn(p, vc[...])
        tot = o[:, 128:]
        outs.append(o[:, :128] / tot)
        l3 = split3(m + jnp.log(tot))
        e = jnp.where(ln == 0, -l3[0], jnp.where(ln == 1, -l3[1], jnp.where(ln == 2, -l3[2], jnp.where(ln == 3, 1.0, 0.0))))
        l_ref[h] = e.astype(bf)
    wide = jnp.where(ln < 64, outs[0], outs[1])
    wide_ref[...] = wide
    o_ref[...] = wide.astype(bf)

def attn_fwd(q, k, v, half, valid, tq=256):
    n, w = q.shape
    np_ = w // 128
    return pl.pallas_call(
        functools.partial(fwd_kernel, half, valid, tq),
        grid=(np_, n // tq),
        out_shape=(jax.ShapeDtypeStruct((n, w), bf), jax.ShapeDtypeStruct((n, w), f32), jax.ShapeDtypeStruct((2 * np_, n, 128), bf)),
        in_specs=[pl.BlockSpec((tq, 128), lambda p, i: (i, p)), pl.BlockSpec((n, 128), lambda p, i: (0, p)), pl.BlockSpec((n, 128), lambda p, i: (0, p))],
        out_specs=[pl.BlockSpec((tq, 128), lambda p, i: (i, p)), pl.BlockSpec((tq, 128), lambda p, i: (i, p)), pl.BlockSpec((2, tq, 128), lambda p, i: (p, i, 0))],
        scratch_shapes=[pltpu.VMEM((2, n, 256), bf), pltpu.VMEM((n, 256), bf)],
        compiler_params=pltpu.CompilerParams(vmem_limit_bytes=60 << 20),
    )(q, k, v)

def bwd_kernel(half, valid, tq, q_ref, k_ref, v_ref, g_ref, o_ref, l_ref, dq_ref, dk_ref, dv_ref, kc, vc, km, dka, dva):
    n = k_ref.shape[0]
    i = pl.program_id(1)
    @pl.when(i == 0)
    def _():
        ln = lanes((n, 128)); pad = lax.rem(rows((n, 128)), half) >= valid
        k = k_ref[...]
        ext = jnp.where(ln < 3, 1.0, jnp.where((ln == 3) & pad, NEG, 0.0)).astype(bf)
        zero = jnp.zeros_like(k)
        kc[:, :128] = k
        kc[:, 128:] = ext
        km[0] = jnp.where(ln < 64, k, zero)
        km[1] = jnp.where(ln < 64, zero, k)
        vc[:, :128] = v_ref[...]
        vc[:, 128:] = ext
        dka[...] = jnp.zeros_like(dka)
        dva[...] = jnp.zeros_like(dva)
    ln = lanes((tq, 128))
    q = q_ref[...] * jnp.asarray(0.125, bf)
    g = g_ref[...]
    go = g.astype(f32) * o_ref[...]
    ps, ds_, qs, gs = [], [], [], []
    dq = jnp.zeros((tq, 128), f32)
    for h in range(2):
        mine = (ln < 64) if h == 0 else (ln >= 64)
        qm = jnp.where(mine, q, jnp.zeros_like(q))
        gm = jnp.where(mine, g, jnp.zeros_like(g))
        d = jnp.sum(jnp.where(mine, go, 0.0), axis=1, keepdims=True)
        d3 = split3(jnp.broadcast_to(d, (tq, 128)))
        de = jnp.where(ln == 0, -d3[0], jnp.where(ln == 1, -d3[1], jnp.where(ln == 2, -d3[2], 0.0))).astype(bf)
        st = nt(kc[...], jnp.concatenate([qm, l_ref[h]], axis=1))
        p = jnp.exp(st)
        dp = nt(vc[...], jnp.concatenate([gm, de], axis=1))
        ds = (p * dp).astype(bf)
        dq = dq + tn(ds, km[h])
        ps.append(p.astype(bf)); ds_.append(ds); qs.append(qm); gs.append(gm)
    dva[...] += nn(ps[0], gs[0]) + nn(ps[1], gs[1])
    dka[...] += nn(ds_[0], qs[0]) + nn(ds_[1], qs[1])
    dq_ref[...] = (dq * 0.125).astype(bf)
    @pl.when(i == pl.num_programs(1) - 1)
    def _():
        dk_ref[...] = dka[...].astype(bf)
        dv_ref[...] = dva[...].astype(bf)

def attn_bwd(q, k, v, g, o, l, half, valid, tq=256):
    n, w = q.shape
    np_ = w // 128
    qs = pl.BlockSpec((tq, 128), lambda p, i: (i, p)); ks = pl.BlockSpec((n, 128), lambda p, i: (0, p))
    return pl.pallas_call(
        functools.partial(bwd_kernel, half, valid, tq),
        grid=(np_, n // tq),
        out_shape=tuple(jax.ShapeDtypeStruct((n, w), bf) for _ in range(3)),
        in_specs=[qs, ks, ks, qs, qs, pl.BlockSpec((2, tq, 128), lambda p, i: (p, i, 0))],
        out_specs=[qs, ks, ks],
        scratch_shapes=[pltpu.VMEM((n, 256), bf), pltpu.VMEM((n, 256), bf), pltpu.VMEM((2, n, 128), bf), pltpu.VMEM((n, 128), f32), pltpu.VMEM((n, 128), f32)],
        compiler_params=pltpu.CompilerParams(vmem_limit_bytes=60 << 20),
    )(q, k, v, g, o, l)
MESH = pl.DeviceIdType.MESH
SEQ = "seq"


class Place:
    def __init__(self, clips):
        self.count = clips.bit_length() - 1
        self.clip = lax.axis_index("clip")
        self.seq = lax.axis_index("seq")
        self.bits = list(reversed(range(self.count))) + [SEQ]

    def mine(self, bit):
        if bit == SEQ:
            return self.seq
        return lax.rem(lax.div(self.clip, 1 << bit), 2)

    def partner(self, bit):
        if bit == SEQ:
            return {"clip": self.clip, "seq": 1 - self.seq}
        return {"clip": self.clip + (1 - 2 * self.mine(bit)) * (1 << bit), "seq": self.seq}

    def index(self, free, flipped=(), without=()):
        out = []
        for bit in self.bits:
            if bit in without:
                continue
            if bit in free:
                out.append(slice(None))
            elif bit in flipped:
                out.append(1 - self.mine(bit))
            else:
                out.append(self.mine(bit))
        return tuple(out)

    def greet(self):
        barrier = pltpu.get_barrier_semaphore()
        for bit in self.bits:
            pl.semaphore_signal(barrier, inc=1, device_id=self.partner(bit), device_id_type=MESH)
        pl.semaphore_wait(barrier, len(self.bits))


def remote(src, dst, sems, partner):
    return pltpu.make_async_remote_copy(
        src_ref=src, dst_ref=dst, send_sem=sems[0], recv_sem=sems[1], device_id=partner, device_id_type=MESH
    )


class Gather:
    def __init__(self, place, shard, out, order, half, sems, local_sem):
        self.place, self.shard, self.out, self.order, self.half = place, shard, out, list(order), half
        self.sems, self.local_sem = sems, local_sem
        self.n_events = len(self.order) + (3 if half is None else 4)
        self.used = 0

    def columns(self, of_seq):
        if self.half is None:
            return self.shard
        return self.shard.at[:, pl.ds(pl.multiple_of(of_seq * self.half, 128), self.half)]

    def copy(self, k, src, dst, bit):
        return remote(src, dst, (self.sems.at[0, k], self.sems.at[1, k]), self.place.partner(bit))

    def local(self):
        return pltpu.make_async_copy(self.columns(self.place.seq), self.out.at[self.place.index(())], self.local_sem)

    def trade(self):
        p = self.place
        return self.copy(0, self.columns(1 - p.seq), self.out.at[p.index(())], SEQ)

    def first_free(self):
        return () if self.half is None else (SEQ,)

    def step(self, k):
        free = self.first_free() + tuple(self.order[:k])
        bit = self.order[k]
        held = self.out.at[self.place.index(free)]
        if k == 0 and self.half is None:
            return self.copy(2 * k + 1, self.shard, held, bit)
        return self.copy(2 * k + 1, held, held, bit)

    def hand(self, k):
        free = self.first_free() + tuple(self.order[:k])
        got = self.out.at[self.place.index(free, flipped=(self.order[k],))]
        return self.copy(2 * k + 2, got, got, 0)

    def hand_own(self):
        own = self.out.at[self.place.index(self.first_free())]
        src = self.shard if self.half is None else own
        return self.copy(2 * len(self.order) + 1, src, own, 0)

    def events(self):
        n = len(self.order)
        run = []
        if self.half is not None:

            def begin():
                self.local().start()
                self.trade().start()

            def first():
                self.local().wait()
                self.trade().wait()
                self.step(0).start()
                self.hand_own().start()

            run += [begin, first]
        else:

            def begin():
                self.local().start()
                self.step(0).start()
                self.hand_own().start()

            run += [begin]
        for k in range(1, n + 1):

            def event(k=k):
                self.step(k - 1).wait_recv()
                if k == 1 and self.half is None:
                    self.local().wait()
                self.hand(k - 1).start()
                if k < n:
                    self.step(k).start()

            run.append(event)

        def finish():
            for k in range(n):
                self.hand(k).wait_recv()
            self.hand_own().wait_recv()
            for k in range(n):
                self.step(k).wait_send()
                self.hand(k).wait_send()
            self.hand_own().wait_send()

        run.append(finish)
        return run


class Scatter:
    def __init__(self, place, parts, out, order, half, acc, recv, last, sems, local_sem):
        self.place, self.parts, self.out, self.order, self.half = place, parts, out, list(order), half
        self.acc, self.recv, self.last, self.sems, self.local_sem = acc, recv, last, sems, local_sem

    def free(self, k):
        return tuple(b for b in self.place.bits if b not in self.order[: k + 1])

    def step(self, k):
        p, bit = self.place, self.order[k]
        free = self.free(k)
        if k == 0:
            src = self.parts.at[p.index(free, flipped=(bit,))]
        else:
            src = self.acc.at[p.index(free, flipped=(bit,), without=(self.order[0],))]
        return remote(src, self.recv[k], (self.sems.at[0, k], self.sems.at[1, k]), p.partner(bit))

    def local(self):
        p = self.place
        return pltpu.make_async_copy(self.parts.at[p.index(self.free(0))], self.acc, self.local_sem)

    def combine(self, k):
        p, n = self.place, len(self.order)
        free = self.free(k)
        total = 1 << len(free)
        recv = self.recv[k]

        def one(i, carry):
            pos, at, full = 0, [], []
            for bit in free:
                at.append(lax.rem(lax.div(i, 1 << pos), 2))
                pos += 1
            named = dict(zip(free, at))
            full = tuple(named[b] if b in named else p.mine(b) for b in p.bits if b != self.order[0])
            value = self.acc[full].astype(f32) + recv[tuple(at)].astype(f32)
            if k == n - 1:
                self.final(named, value)
            else:
                self.acc[full] = value.astype(self.acc.dtype)
            return carry

        if total == 1:
            one(0, 0)
        else:
            lax.fori_loop(0, total, one, 0)

    def final(self, named, value):
        if self.half is None:
            self.out[...] = value
        else:
            self.last[0, named[SEQ]] = value.astype(bf)

    def trade(self):
        p, n = self.place, len(self.order)
        return remote(self.last.at[0, 1 - p.seq], self.last.at[1, 0], (self.sems.at[0, n], self.sems.at[1, n]), p.partner(SEQ))

    def events(self):
        n = len(self.order)
        run = []

        def begin():
            self.step(0).start()
            self.local().start()

        run.append(begin)
        for k in range(n):

            def event(k=k):
                if k == 0:
                    self.local().wait()
                self.step(k).wait_recv()
                self.combine(k)
                if k + 1 < n:
                    self.step(k + 1).start()
                elif self.half is not None:
                    self.trade().start()

            run.append(event)

        def finish():
            for k in range(n):
                self.step(k).wait_send()
            if self.half is not None:
                self.trade().wait()
                s = self.place.seq
                own, other = self.last[0, s].astype(f32), self.last[1, 0].astype(f32)

                @pl.when(s == 0)
                def _():
                    self.out[:, : self.half] = own
                    self.out[:, self.half :] = other

                @pl.when(s == 1)
                def _():
                    self.out[:, : self.half] = other
                    self.out[:, self.half :] = own

        run.append(finish)
        return run


def orders(count):
    high = list(reversed(range(2, count)))
    return ([*high, 1, SEQ], [*high, SEQ, 1], [1, SEQ, *high])


def run_round_robin(programs):
    most = max(len(p) for p in programs)
    for i in range(most):
        for p in programs:
            if i < len(p):
                p[i]()


def gather_all(clips, full, halves, rows):
    count = clips.bit_length() - 1
    nbits = count + 1
    nf, nh = len(full), len(halves)

    def kernel(*refs):
        ins, outs = refs[: nf + nh + 1], refs[nf + nh + 1 : 2 * (nf + nh + 1)]
        sems, local_sems, row_sems = refs[2 * (nf + nh + 1) :]
        place = Place(clips)
        place.greet()
        row_out = outs[-1]
        give = remote(ins[-1], row_out.at[place.seq], (row_sems.at[0], row_sems.at[1]), place.partner(SEQ))
        give.start()
        keep = pltpu.make_async_copy(ins[-1], row_out.at[place.seq], row_sems.at[2])
        keep.start()
        abc = orders(count)
        programs = []
        for j in range(nh):
            order = [b for b in abc[(0, 2, 2)[j % 3]] if b != SEQ]
            programs.append(Gather(place, ins[nf + j], outs[nf + j], order, halves[j].shape[1] // 2, sems.at[nf + j], local_sems.at[nf + j]).events())
        for j in range(nf):
            programs.append(Gather(place, ins[j], outs[j], abc[j % 3], None, sems.at[j], local_sems.at[j]).events())
        run_round_robin(programs)
        keep.wait()
        give.wait()

    two = (2,) * nbits
    any_spec = pl.BlockSpec(memory_space=pl.ANY)
    vmem = pl.BlockSpec(memory_space=pltpu.VMEM)
    out = pl.pallas_call(
        kernel,
        out_shape=tuple(jax.ShapeDtypeStruct(two + a.shape, a.dtype) for a in full)
        + tuple(jax.ShapeDtypeStruct(two + (a.shape[0], a.shape[1] // 2), a.dtype) for a in halves)
        + (jax.ShapeDtypeStruct((2,) + rows.shape, rows.dtype),),
        in_specs=[vmem] * (nf + nh + 1),
        out_specs=(any_spec,) * (nf + nh + 1),
        scratch_shapes=[
            pltpu.SemaphoreType.DMA((nf + nh, 2, 2 * nbits + 2)),
            pltpu.SemaphoreType.DMA((nf + nh,)),
            pltpu.SemaphoreType.DMA((3,)),
        ],
        compiler_params=pltpu.CompilerParams(collective_id=0, has_side_effects=True),
    )(*full, *halves, rows)
    whole = [o.reshape((-1, a.shape[1])) for o, a in zip(out[:nf], full)]
    half = [o.reshape((-1, a.shape[1] // 2)) for o, a in zip(out[nf : nf + nh], halves)]
    return whole, half, out[-1].reshape((-1, rows.shape[1]))


def scatter_all(clips, full, halves, rows):
    count = clips.bit_length() - 1
    nbits = count + 1
    devices = 2 * clips
    nf, nh = len(full), len(halves)
    two = (2,) * nbits
    parts = [a.reshape(two + (a.shape[0] // devices, a.shape[1])) for a in (*full, *halves)]
    rows = rows.reshape((2, rows.shape[0] // 2, rows.shape[1]))
    abc = [[0, *reversed(o)] for o in orders(count)]

    def order_of(j):
        if j < nf:
            return abc[j % 3]
        return [b for b in abc[(0, 2, 2)[(j - nf) % 3]] if b != SEQ]

    scratch = []
    for j, a in enumerate(parts):
        shard = a.shape[nbits:]
        scratch.append(pltpu.VMEM(two[:-1] + shard, a.dtype))
        for k in range(len(order_of(j))):
            scratch.append(pltpu.VMEM(two[: nbits - 1 - k] + shard, a.dtype))
        scratch.append(pltpu.VMEM((2, 2) + shard, bf) if j >= nf else pltpu.VMEM((8, 128), f32))

    def kernel(*refs):
        n = nf + nh
        ins, outs = refs[: n + 1], refs[n + 1 : 2 * n + 2]
        bufs, (sems, local_sems, row_sems) = list(refs[2 * n + 2 : -3]), refs[-3:]
        place = Place(clips)
        place.greet()
        give = remote(ins[-1].at[1 - place.seq], outs[-1], (row_sems.at[0], row_sems.at[1]), place.partner(SEQ))
        give.start()
        programs = []
        for j in range(n):
            order = order_of(j)
            acc = bufs.pop(0)
            recv = [bufs.pop(0) for _ in order]
            last = bufs.pop(0)
            half = None if j < nf else parts[j].shape[-1]
            programs.append(Scatter(place, ins[j], outs[j], order, half, acc, recv, last, sems.at[j], local_sems.at[j]).events())
        run_round_robin(programs)
        give.wait()

    any_spec = pl.BlockSpec(memory_space=pl.ANY)
    vmem = pl.BlockSpec(memory_space=pltpu.VMEM)
    out = pl.pallas_call(
        kernel,
        out_shape=tuple(
            jax.ShapeDtypeStruct((a.shape[-2], a.shape[-1] * (2 if j >= nf else 1)), f32) for j, a in enumerate(parts)
        )
        + (jax.ShapeDtypeStruct(rows.shape[1:], rows.dtype),),
        in_specs=[any_spec] * (nf + nh + 1),
        out_specs=(vmem,) * (nf + nh) + (any_spec,),
        scratch_shapes=scratch
        + [
            pltpu.SemaphoreType.DMA((nf + nh, 2, nbits + 1)),
            pltpu.SemaphoreType.DMA((nf + nh,)),
            pltpu.SemaphoreType.DMA((2,)),
        ],
        compiler_params=pltpu.CompilerParams(collective_id=1, has_side_effects=True, vmem_limit_bytes=60 << 20),
    )(*parts, rows)
    return out[:nf], out[nf : nf + nh], out[-1]


epsilon = 1e-05
root_half = 0.7071067811865476


def pad_rows(x, to):
    return jnp.pad(x, ((0, to - x.shape[0]), (0, 0)))


def norm_parts(rows_in):
    center = rows_in - jnp.mean(rows_in, axis=-1, keepdims=True)
    scale = lax.rsqrt(jnp.mean(center * center, axis=-1, keepdims=True) + epsilon)
    return center * scale, scale


def norm_back(gy, gain, xhat, scale):
    gt = gy * gain
    return scale * (gt - jnp.mean(gt, axis=-1, keepdims=True) - xhat * jnp.mean(gt * xhat, axis=-1, keepdims=True))


def per_device(
    clips,
    frames,
    norm1_gain,
    norm1_shift,
    query_weight,
    query_bias,
    key_weight,
    value_weight,
    value_bias,
    out_weight,
    out_bias,
    norm2_gain,
    norm2_shift,
    hidden_weight,
    hidden_bias,
    output_weight,
    output_bias,
    out_grad,
):
    seq = lax.axis_index("seq")
    valid, width = frames.shape[1], frames.shape[2]
    half = -(-valid // 256) * 256
    cols = width // 2
    devices = 2 * clips
    vectors = (norm1_gain, norm1_shift, query_bias, value_bias, out_bias, norm2_gain, norm2_shift, hidden_bias, output_bias)
    sizes = [v.shape[0] for v in vectors]
    packed = jnp.pad(jnp.concatenate(vectors), (0, 1024 - sum(sizes))).reshape(8, 128)
    own = pad_rows(frames[0], half)
    (w_hidden, w_output, w_out, small), (w_query, w_key, w_value), both = gather_all(
        clips, [hidden_weight, output_weight, out_weight, packed], [query_weight, key_weight, value_weight], own
    )
    small = small.reshape(devices, 1024).astype(f32)
    unpacked, at = [], 0
    for size in sizes:
        unpacked.append(small[:, at : at + size].reshape(-1))
        at += size
    gain_one, shift_one, b_query, b_value, b_out, gain_two, shift_two, b_hidden, b_output = unpacked
    b_query = lax.dynamic_slice_in_dim(b_query, seq * cols, cols)
    b_value = lax.dynamic_slice_in_dim(b_value, seq * cols, cols)

    xhat_both, scale_both = norm_parts(both.astype(f32))
    normed = (xhat_both * gain_one + shift_one).astype(bf)
    query = (nn(normed, w_query) + b_query).astype(bf)
    key = nn(normed, w_key).astype(bf)
    value = (nn(normed, w_value) + b_value).astype(bf)
    attended_cols, wide_cols, log_cols = attn_fwd(query, key, value, half, valid)

    def trade(x):
        mine = lax.dynamic_slice_in_dim(x, seq * half, half)
        give = lax.dynamic_slice_in_dim(x, (1 - seq) * half, half)
        got = lax.ppermute(give, "seq", [(0, 1), (1, 0)])
        return jnp.where(seq == 0, jnp.concatenate([mine, got], 1), jnp.concatenate([got, mine], 1))

    def trade_back(x):
        mine = lax.dynamic_slice_in_dim(x, seq * cols, cols, 1)
        give = lax.dynamic_slice_in_dim(x, (1 - seq) * cols, cols, 1)
        got = lax.ppermute(give, "seq", [(0, 1), (1, 0)])
        return jnp.where(seq == 0, jnp.concatenate([mine, got], 0), jnp.concatenate([got, mine], 0))

    attended = trade(attended_cols)
    hidden_in = own.astype(f32) + nn(attended, w_out) + b_out
    xhat_two, scale_two = norm_parts(hidden_in)
    normed_two = (xhat_two * gain_two + shift_two).astype(bf)
    pre_act = nn(normed_two, w_hidden) + b_hidden
    cdf = 0.5 * (1.0 + lax.erf(pre_act * root_half))
    acted = (pre_act * cdf).astype(bf)
    encoded = (hidden_in + nn(acted, w_output) + b_output).astype(bf)[:valid]

    grad_ff = pad_rows(out_grad[0], half)
    grad_out = grad_ff.astype(f32)
    grad_w_output = tn(acted, grad_ff)
    slope = cdf + pre_act * jnp.exp(-0.5 * pre_act * pre_act) * 0.3989422804014327
    grad_pre = (nt(grad_ff, w_output) * slope).astype(bf)
    grad_w_hidden = tn(normed_two, grad_pre)
    gy_two = nt(grad_pre, w_hidden)
    grad_hidden_in = grad_out + norm_back(gy_two, gain_two, xhat_two, scale_two)
    grad_branch = grad_hidden_in.astype(bf)
    grad_w_out = tn(attended, grad_branch)
    grad_attended = nt(grad_branch, w_out).astype(bf)

    query_grad, key_grad, value_grad = attn_bwd(
        query, key, value, trade_back(grad_attended), wide_cols, log_cols, half, valid
    )
    grad_w_query = tn(normed, query_grad)
    grad_w_key = tn(normed, key_grad)
    grad_w_value = tn(normed, value_grad)
    gy_one = nt(query_grad, w_query) + nt(key_grad, w_key) + nt(value_grad, w_value)

    def sums(x):
        return jnp.sum(x.astype(f32), axis=0)

    def spread(x):
        return lax.dynamic_update_slice_in_dim(jnp.zeros((width,), f32), x, seq * cols, 0)

    vector_sums = (
        sums(gy_one * xhat_both),
        sums(gy_one),
        spread(sums(query_grad)),
        spread(sums(value_grad)),
        sums(grad_branch),
        sums(gy_two * xhat_two),
        sums(gy_two),
        sums(grad_pre),
        sums(grad_ff),
    )
    packed_sums = jnp.concatenate([v.reshape(devices, -1) for v in vector_sums], axis=1)
    packed_sums = jnp.pad(packed_sums, ((0, 0), (0, 1024 - packed_sums.shape[1]))).reshape(devices * 8, 128)
    (own_hidden, own_output, own_out, own_small), (own_query, own_key, own_value), gy_got = scatter_all(
        clips,
        [grad_w_hidden.astype(bf), grad_w_output.astype(bf), grad_w_out.astype(bf), packed_sums],
        [grad_w_query.astype(bf), grad_w_key.astype(bf), grad_w_value.astype(bf)],
        gy_one.astype(bf),
    )
    gy_mine = lax.dynamic_slice_in_dim(gy_one, seq * half, half) + gy_got.astype(f32)
    xhat_one, scale_one = norm_parts(own.astype(f32))
    frames_grad = (grad_hidden_in + norm_back(gy_mine, gain_one, xhat_one, scale_one)).astype(bf)[:valid]

    own_small = own_small.reshape(-1)
    owned, at = [], 0
    for size in sizes:
        owned.append(own_small[at : at + size])
        at += size
    return (
        encoded[None],
        frames_grad[None],
        owned[0],
        owned[1],
        own_query,
        owned[2],
        own_key,
        own_value,
        owned[3],
        own_out,
        owned[4],
        owned[5],
        owned[6],
        own_hidden,
        owned[7],
        own_output,
        owned[8],
    )


def solution(mesh):
    rows, vector, matrix = P("clip", "seq", None), P(("clip", "seq")), P(("clip", "seq"), None)
    placed = (
        rows,
        vector,
        vector,
        matrix,
        vector,
        matrix,
        matrix,
        vector,
        matrix,
        vector,
        vector,
        vector,
        matrix,
        vector,
        matrix,
        vector,
        rows,
    )
    weights = placed[1:-1]
    return jax.shard_map(
        functools.partial(per_device, mesh.shape["clip"]),
        mesh=mesh,
        in_specs=placed,
        out_specs=(rows, rows) + weights,
        check_vma=False,
    )
```

```python
import functools

import jax
import jax.numpy as jnp
from jax import lax
from jax.experimental import pallas as pl
from jax.experimental.pallas import tpu as pltpu
from jax.sharding import PartitionSpec as P

bf, f32 = jnp.bfloat16, jnp.float32
MESH = pl.DeviceIdType.MESH
SEQ = "seq"
ANY = pl.BlockSpec(memory_space=pl.ANY)
VMEM = pl.BlockSpec(memory_space=pltpu.VMEM)
DMA = pltpu.SemaphoreType.DMA
SIDE = dict(has_side_effects=True, vmem_limit_bytes=62 << 20)


class Place:
    def __init__(self, clips):
        self.count = clips.bit_length() - 1
        self.clip = lax.axis_index("clip")
        self.seq = lax.axis_index("seq")

    def mine(self, bit):
        if bit == SEQ:
            return self.seq
        return lax.rem(lax.div(self.clip, 1 << bit), 2)

    def partner(self, bit):
        if bit == SEQ:
            return {"clip": self.clip, "seq": 1 - self.seq}
        return {"clip": self.clip + (1 - 2 * self.mine(bit)) * (1 << bit), "seq": self.seq}

    def index(self, dims, free, flipped=None):
        return tuple(slice(None) if b in free else 1 - self.mine(b) if b == flipped else self.mine(b) for b in dims)

    def greet(self):
        barrier = pltpu.get_barrier_semaphore()
        bits = all_bits(self.count)
        for bit in bits:
            pl.semaphore_signal(barrier, inc=1, device_id=self.partner(bit), device_id_type=MESH)
        pl.semaphore_wait(barrier, len(bits))


def all_bits(count):
    return [*reversed(range(count)), SEQ]


def high_bits(count):
    return list(reversed(range(2, count)))


def twos(bits):
    return (2,) * len(bits)


def remote(src, dst, sems, partner):
    return pltpu.make_async_remote_copy(
        src_ref=src, dst_ref=dst, send_sem=sems[0], recv_sem=sems[1], device_id=partner, device_id_type=MESH
    )


class Gather:
    def __init__(self, place, src, out, dims, start, order, sems, hand=True, half=None):
        self.place, self.src, self.out, self.dims, self.start = place, src, out, dims, tuple(start)
        self.order, self.sems, self.hands, self.half = list(order), sems, hand, half

    @staticmethod
    def semaphores(order):
        return DMA((2, 2 * len(order) + 4))

    def copy(self, k, src, dst, bit):
        return remote(src, dst, (self.sems.at[0, k], self.sems.at[1, k]), self.place.partner(bit))

    def columns(self, of_seq):
        if self.half is None:
            return self.src
        return self.src.at[:, pl.ds(pl.multiple_of(of_seq * self.half, 128), self.half)]

    def local(self):
        free = () if self.half else self.start
        at = self.out.at[self.place.index(self.dims, free)]
        return pltpu.make_async_copy(self.columns(self.place.seq), at, self.sems.at[0, 0])

    def trade(self):
        p = self.place
        return self.copy(1, self.columns(1 - p.seq), self.out.at[p.index(self.dims, ())], SEQ)

    def step(self, k):
        held = self.out.at[self.place.index(self.dims, self.start + tuple(self.order[:k]))]
        src = self.src if k == 0 and self.half is None else held
        return self.copy(2 * k + 2, src, held, self.order[k])

    def hand(self, k):
        if k == 0:
            at = self.out.at[self.place.index(self.dims, self.start)]
            return self.copy(2 * len(self.order) + 2, self.src if self.half is None else at, at, 0)
        free = self.start + tuple(self.order[: k - 1])
        at = self.out.at[self.place.index(self.dims, free, self.order[k - 1])]
        return self.copy(2 * k + 1, at, at, 0)

    def events(self):
        n = len(self.order)

        def begin():
            self.local().start()
            if self.half is not None:
                self.trade().start()
            else:
                self.step(0).start()
                if self.hands:
                    self.hand(0).start()

        def traded():
            self.local().wait()
            self.trade().wait()
            self.step(0).start()
            self.hand(0).start()

        def arrived(k):
            self.step(k).wait_recv()
            if k == 0 and self.half is None:
                self.local().wait()
            if self.hands:
                self.hand(k + 1).start()
            if k + 1 < n:
                self.step(k + 1).start()

        def finish():
            for k in range(n):
                self.step(k).wait_send()
            if self.hands:
                for k in range(n + 1):
                    self.hand(k).wait()

        run = [begin] + ([traded] if self.half is not None else [])
        return run + [functools.partial(arrived, k) for k in range(n)] + [finish]


class Scatter:
    def __init__(self, place, parts, dims, order, acc, recv, sems, final):
        self.place, self.parts, self.dims, self.order = place, parts, list(dims), list(order)
        self.acc, self.recv, self.sems, self.final = acc, recv, sems, final

    @staticmethod
    def scratch(dims, order, shard, dtype):
        n = len(dims)
        bufs = [pltpu.VMEM((2,) * (n - 1) + shard, dtype)]
        bufs += [pltpu.VMEM((2,) * (n - 1 - k) + shard, dtype) for k in range(len(order))]
        return bufs + [DMA((2, len(order) + 1))]

    def free(self, k):
        return tuple(b for b in self.dims if b not in self.order[: k + 1])

    def step(self, k):
        p, bit = self.place, self.order[k]
        if k == 0:
            src = self.parts.at[p.index(self.dims, self.free(k), bit)]
        else:
            src = self.acc.at[p.index([b for b in self.dims if b != self.order[0]], self.free(k), bit)]
        return remote(src, self.recv[k], (self.sems.at[0, k], self.sems.at[1, k]), p.partner(bit))

    def local(self):
        src = self.parts.at[self.place.index(self.dims, self.free(0))]
        return pltpu.make_async_copy(src, self.acc, self.sems.at[0, len(self.order)])

    def combine(self, k):
        p, free = self.place, self.free(k)

        def one(i, carry):
            at = {b: lax.rem(lax.div(i, 1 << pos), 2) for pos, b in enumerate(reversed(free))}
            full = tuple(at[b] if b in at else p.mine(b) for b in self.dims if b != self.order[0])
            value = self.acc[full].astype(f32) + self.recv[k][tuple(at[b] for b in free)].astype(f32)
            if k == len(self.order) - 1:
                self.final(tuple(at[b] for b in free), value)
            else:
                self.acc[full] = value.astype(self.acc.dtype)
            return carry

        if free:
            lax.fori_loop(0, 1 << len(free), one, 0)
        else:
            one(0, 0)

    def events(self):
        n = len(self.order)

        def begin():
            self.step(0).start()
            self.local().start()

        def arrived(k):
            if k == 0:
                self.local().wait()
            self.step(k).wait_recv()
            self.combine(k)
            if k + 1 < n:
                self.step(k + 1).start()

        def finish():
            for k in range(n):
                self.step(k).wait_send()

        return [begin] + [functools.partial(arrived, k) for k in range(n)] + [finish]


def round_robin(programs):
    for i in range(max(len(p) for p in programs)):
        for p in programs:
            if i < len(p):
                p[i]()


def at_steps(here, plan):
    for step in sorted({s for s, _ in plan}):

        @pl.when(here == step)
        def _(step=step):
            for s, event in plan:
                if s == step:
                    event()


def first_gather(clips, halves, small, ahead, frames):
    count = clips.bit_length() - 1
    bits, high = all_bits(count), high_bits(count)
    nh, na = len(halves), len(ahead)
    around = [*high, 1]

    def kernel(*refs):
        n = nh + na + 2
        ins, outs, sems = refs[:n], refs[n : 2 * n], refs[2 * n :]
        place = Place(clips)
        place.greet()
        give = remote(ins[-1], outs[-1].at[place.seq], (sems[-1].at[0], sems[-1].at[1]), place.partner(SEQ))
        keep = pltpu.make_async_copy(ins[-1], outs[-1].at[place.seq], sems[-1].at[2])
        programs = []
        for j, a in enumerate(halves):
            programs.append(Gather(place, ins[j], outs[j], bits, (SEQ,), around, sems[j], half=a.shape[1] // 2).events())
        programs.append(Gather(place, ins[nh], outs[nh], bits, (), [SEQ, *around], sems[nh]).events())
        for j in range(nh + 1, nh + 1 + na):
            programs.append(Gather(place, ins[j], outs[j], high, (), high, sems[j], hand=False).events())
        for p in programs:
            p.pop(0)()
        give.start()
        keep.start()
        round_robin(programs)
        keep.wait()
        give.wait()

    def like(lead, a, cols=None):
        return jax.ShapeDtypeStruct(lead + (a.shape[0], cols or a.shape[1]), a.dtype)

    out = pl.pallas_call(
        kernel,
        out_shape=tuple(like(twos(bits), a, a.shape[1] // 2) for a in halves)
        + (like(twos(bits), small),)
        + tuple(like(twos(high), a) for a in ahead)
        + (like((2,), frames),),
        in_specs=[VMEM] * (nh + na + 2),
        out_specs=(ANY,) * (nh + na + 2),
        scratch_shapes=[Gather.semaphores(around)] * nh
        + [Gather.semaphores([SEQ, *around])]
        + [Gather.semaphores(high)] * na
        + [DMA((3,))],
        compiler_params=pltpu.CompilerParams(collective_id=0, **SIDE),
    )(*halves, small, *ahead, frames)
    return [o.reshape((-1, o.shape[-1])) for o in out[:nh]], out[nh], out[nh + 1 : -1], out[-1]


def last_scatter(clips, halves, small, ahead, rows):
    count = clips.bit_length() - 1
    bits, high = all_bits(count), high_bits(count)
    devices = 2 * clips
    nh, na = len(halves), len(ahead)
    low = list(reversed(high))
    around = [0, 1, *low]
    parts = [a.reshape(twos(bits) + (a.shape[0] // devices, a.shape[1])) for a in (*halves, small)] + list(ahead)
    plans = [(bits, around)] * nh + [(bits, [0, SEQ, 1, *low])] + [(high, low)] * na
    n = nh + na + 1
    scratch, counts = [], []
    for j, (a, (dims, order)) in enumerate(zip(parts, plans)):
        shard = a.shape[len(dims) :]
        new = Scatter.scratch(dims, order, shard, a.dtype)
        if j < nh:
            new += [pltpu.VMEM((2,) + shard, bf), pltpu.VMEM(shard, bf), DMA((2,))]
        scratch += new
        counts.append(len(new))

    def kernel(*refs):
        ins, outs, bufs = refs[: n + 1], refs[n + 1 : 2 * n + 2], refs[2 * n + 2 :]
        place = Place(clips)
        place.greet()
        swap = remote(ins[-1].at[1 - place.seq], outs[-1], (bufs[-1].at[0], bufs[-1].at[1]), place.partner(SEQ))
        programs, at = [], 0
        for j, (dims, order) in enumerate(plans):
            mine, at = bufs[at : at + counts[j]], at + counts[j]
            acc, recv, sems = mine[0], mine[1 : 1 + len(order)], mine[1 + len(order)]
            if j < nh:
                last, other, trade_sems = mine[2 + len(order) :]

                def final(where, value, last=last):
                    last[where] = value.astype(bf)

                def trade(last=last, other=other, sems=trade_sems):
                    return remote(last.at[1 - place.seq], other, (sems.at[0], sems.at[1]), place.partner(SEQ))

                def close(last=last, other=other, trade=trade, out=outs[j], width=parts[j].shape[-1]):
                    trade().wait()
                    mine, theirs = last[place.seq].astype(f32), other[...].astype(f32)
                    first = place.seq == 0
                    out[:, :width] = jnp.where(first, mine, theirs)
                    out[:, width:] = jnp.where(first, theirs, mine)

                events = Scatter(place, ins[j], dims, order, acc, recv, sems, final).events()
                events.insert(-1, lambda trade=trade: trade().start())
                events.append(close)
            else:

                def final(where, value, out=outs[j]):
                    out[...] = value

                events = Scatter(place, ins[j], dims, order, acc, recv, sems, final).events()
            programs.append(events)
        for p in programs:
            p.pop(0)()
        swap.start()
        round_robin(programs)
        swap.wait()

    out = pl.pallas_call(
        kernel,
        out_shape=tuple(
            jax.ShapeDtypeStruct((a.shape[-2], a.shape[-1] * (2 if j < nh else 1)), f32) for j, a in enumerate(parts)
        )
        + (jax.ShapeDtypeStruct(rows.shape[1:], rows.dtype),),
        in_specs=[ANY] * (n + 1),
        out_specs=(VMEM,) * n + (ANY,),
        scratch_shapes=scratch + [DMA((2,))],
        compiler_params=pltpu.CompilerParams(collective_id=3, **SIDE),
    )(*parts, rows)
    return out[:nh], out[nh], out[nh + 1 : -1], out[-1]
NEG = -1e30
TILE = 256


def nt(a, b):
    return lax.dot_general(a, b, (((1,), (1,)), ((), ())), preferred_element_type=f32)


def nn(a, b):
    return lax.dot_general(a, b, (((1,), (0,)), ((), ())), preferred_element_type=f32)


def tn(a, b):
    return lax.dot_general(a, b, (((0,), (0,)), ((), ())), preferred_element_type=f32)


def lanes(shape):
    return lax.broadcasted_iota(jnp.int32, shape, 1)


def padding(shape, half, valid):
    return lax.rem(lax.broadcasted_iota(jnp.int32, shape, 0), half) >= valid


def in_lanes(ln, pieces):
    out = 0.0
    for i, piece in reversed(list(enumerate(pieces))):
        out = jnp.where(ln == i, piece, out)
    return out.astype(bf)


def three(x):
    high = x.astype(bf).astype(f32)
    mid = (x - high).astype(bf).astype(f32)
    return [-high, -mid, -(x - high - mid)]


def attn_fwd(clips, q, k, v, whole, ahead, half, valid):
    n, w = q.shape
    pairs, tiles = w // 128, n // TILE
    count = clips.bit_length() - 1
    bits, high = all_bits(count), high_bits(count)
    arrays = [*ahead, *whole]
    starts = [high] * len(ahead) + [[]] * len(whole)
    orders = [[1, SEQ] if j % 2 == 0 else [SEQ, 1] for j in range(len(ahead))] + [[1, SEQ, *high]] * len(whole)
    na = len(arrays)

    def kernel(q_ref, k_ref, v_ref, *refs):
        srcs, (att_out, wide_ref, l_ref), outs = refs[:na], refs[na : na + 3], refs[na + 3 : 2 * na + 3]
        kc, vc, att, att_sems = refs[2 * na + 3 : 2 * na + 7]
        sems = refs[2 * na + 7 :]
        pair, tile = pl.program_id(0), pl.program_id(1)
        here = pair * tiles + tile
        place = Place(clips)

        def att_copies(p):
            cols = pl.ds(pl.multiple_of(place.seq * w + p * 128, 128), 128)
            own = pltpu.make_async_copy(
                att.at[pl.ds(pl.multiple_of(place.seq * half, half), half), pl.ds(p * 128, 128)],
                att_out.at[:, cols],
                att_sems.at[0, p],
            )
            give = remote(
                att.at[pl.ds(pl.multiple_of((1 - place.seq) * half, half), half), pl.ds(p * 128, 128)],
                att_out.at[:, cols],
                (att_sems.at[1, p], att_sems.at[2, p]),
                place.partner(SEQ),
            )
            return own, give

        def start_att(p):
            for c in att_copies(p):
                c.start()

        programs = [
            Gather(place, srcs[j], outs[j], bits, starts[j], orders[j], sems[j]).events() for j in range(na)
        ]
        last = pairs * tiles - 1
        begin = [(0, place.greet)]
        ends = []
        for j, p in enumerate(programs):
            begin.append((0, p[0]))
            waits = p[1:-1]
            for k, event in enumerate(waits):
                ends.append((min(last, (k + 1) * last // (len(waits) + 1)) if k + 1 < len(waits) else last, event))
            ends.append((last, p[-1]))
        at_steps(here, begin)

        @pl.when(tile == 0)
        def _():
            ln = lanes((n, 128))
            kk = k_ref[...]
            ext = in_lanes(ln, [jnp.where(padding((n, 128), half, valid), NEG, 0.0)])
            zero = jnp.zeros_like(kk)
            kc[0, :, :128] = jnp.where(ln < 64, kk, zero)
            kc[1, :, :128] = jnp.where(ln < 64, zero, kk)
            kc[0, :, 128:] = ext
            kc[1, :, 128:] = ext
            vc[:, :128] = v_ref[...]
            vc[:, 128:] = jnp.ones((n, 128), bf)

        ln = lanes((TILE, 128))
        qc = jnp.concatenate([q_ref[...] * jnp.asarray(0.125, bf), in_lanes(ln, [1.0])], axis=1)
        heads = []
        for h in range(2):
            s = nt(qc, kc[h])
            top = jnp.max(s, axis=1, keepdims=True)
            o = nn(jnp.exp(s - top).astype(bf), vc[...])
            total = o[:, 128:]
            heads.append(o[:, :128] / total)
            l_ref[h] = in_lanes(ln, three(top + jnp.log(total)) + [1.0])
        wide = jnp.where(ln < 64, heads[0], heads[1])
        wide_ref[...] = wide
        for p in range(pairs):

            @pl.when(pair == p)
            def _(p=p):
                att[pl.ds(pl.multiple_of(tile * TILE, TILE), TILE), p * 128 : (p + 1) * 128] = wide.astype(bf)

        at_steps(here, [((p + 1) * tiles - 1, functools.partial(start_att, p)) for p in range(pairs)])
        at_steps(here, ends)

        @pl.when(here == last)
        def _():
            for p in range(pairs):
                for c in att_copies(p):
                    c.wait()

    tile_spec = pl.BlockSpec((TILE, 128), lambda p, i: (i, p))
    all_spec = pl.BlockSpec((n, 128), lambda p, i: (0, p))
    out = pl.pallas_call(
        kernel,
        grid=(pairs, tiles),
        out_shape=(
            jax.ShapeDtypeStruct((half, 2 * w), bf),
            jax.ShapeDtypeStruct((n, w), f32),
            jax.ShapeDtypeStruct((2 * pairs, n, 128), bf),
        )
        + tuple(jax.ShapeDtypeStruct(twos(bits) + a.shape[len(s) :], a.dtype) for a, s in zip(arrays, starts)),
        in_specs=[tile_spec, all_spec, all_spec] + [VMEM] * na,
        out_specs=(ANY, tile_spec, pl.BlockSpec((2, TILE, 128), lambda p, i: (p, i, 0))) + (ANY,) * na,
        scratch_shapes=[pltpu.VMEM((2, n, 256), bf), pltpu.VMEM((n, 256), bf), pltpu.VMEM((n, w), bf), DMA((3, pairs))]
        + [Gather.semaphores(o) for o in orders],
        compiler_params=pltpu.CompilerParams(collective_id=1, **SIDE),
    )(q, k, v, *arrays)
    return out[0], out[1], out[2], [o.reshape((-1, o.shape[-1])) for o in out[3:]]


def attn_bwd(clips, q, k, v, g, wide, logs, ahead, whole, half, valid):
    n, w = q.shape
    pairs, tiles = w // 128, n // TILE
    count = clips.bit_length() - 1
    bits, high = all_bits(count), high_bits(count)
    devices = 2 * clips
    parts = [a.reshape(twos(bits) + (a.shape[0] // devices, a.shape[1])) for a in (*ahead, *whole)]
    orders = [[0, SEQ, 1] if j % 2 == 0 else [0, 1, SEQ] for j in range(len(ahead))] + [[0, *reversed(high), SEQ, 1]] * len(whole)
    na = len(parts)
    scratch, counts = [], []
    for a, order in zip(parts, orders):
        new = Scatter.scratch(bits, order, a.shape[len(bits) :], a.dtype)
        scratch += new
        counts.append(len(new))

    def kernel(q_ref, k_ref, v_ref, g_in, o_ref, l_ref, *refs):
        srcs, (dq_ref, dk_ref, dv_ref), outs = refs[:na], refs[na : na + 3], refs[na + 3 : 2 * na + 3]
        kc, vc, km, dka, dva, g_all, g_sems = refs[2 * na + 3 : 2 * na + 10]
        bufs = refs[2 * na + 10 :]
        pair, tile = pl.program_id(0), pl.program_id(1)
        here = pair * tiles + tile
        last = pairs * tiles - 1
        place = Place(clips)

        def g_copies(p):
            own = pltpu.make_async_copy(
                g_in.at[:, pl.ds(pl.multiple_of(place.seq * w + p * 128, 128), 128)],
                g_all.at[p, place.seq],
                g_sems.at[0, p],
            )
            give = remote(
                g_in.at[:, pl.ds(pl.multiple_of((1 - place.seq) * w + p * 128, 128), 128)],
                g_all.at[p, place.seq],
                (g_sems.at[1, p], g_sems.at[2, p]),
                place.partner(SEQ),
            )
            return own, give

        def start_g():
            for p in range(pairs):
                for c in g_copies(p):
                    c.start()

        def wait_g(p):
            for c in g_copies(p):
                c.wait()

        begin, ends, at = [(0, place.greet), (0, start_g)], [], 0
        for j, order in enumerate(orders):
            mine, at = bufs[at : at + counts[j]], at + counts[j]

            def final(where, value, out=outs[j]):
                out[where if where else ...] = value.astype(out.dtype)

            program = Scatter(place, srcs[j], bits, order, mine[0], mine[1:-1], mine[-1], final).events()
            begin.append((0, program[0]))
            waits = program[1:-1]
            if j < len(ahead):
                when = [3 + j, 13 + j, last]
            else:
                when = [min(last, 5 + 3 * k) for k in range(len(waits))]
            ends += list(zip(when, waits)) + [(last, program[-1])]
        ends.sort(key=lambda e: e[0])
        at_steps(here, begin + [(p * tiles, functools.partial(wait_g, p)) for p in range(pairs)])

        @pl.when(tile == 0)
        def _():
            ln = lanes((n, 128))
            kk = k_ref[...]
            ext = in_lanes(ln, [1.0, 1.0, 1.0, jnp.where(padding((n, 128), half, valid), NEG, 0.0)])
            zero = jnp.zeros_like(kk)
            kc[:, :128] = kk
            kc[:, 128:] = ext
            km[0] = jnp.where(ln < 64, kk, zero)
            km[1] = jnp.where(ln < 64, zero, kk)
            vc[:, :128] = v_ref[...]
            vc[:, 128:] = ext
            dka[...] = jnp.zeros_like(dka)
            dva[...] = jnp.zeros_like(dva)

        ln = lanes((TILE, 128))
        q = q_ref[...] * jnp.asarray(0.125, bf)
        per = half // TILE
        g = g_all[pair, lax.div(tile, per), pl.ds(pl.multiple_of(lax.rem(tile, per) * TILE, TILE), TILE), :]
        go = g.astype(f32) * o_ref[...]
        probs, scores, qs, gs = [], [], [], []
        dq = jnp.zeros((TILE, 128), f32)
        for h in range(2):
            mine = (ln < 64) if h == 0 else (ln >= 64)
            qm = jnp.where(mine, q, jnp.zeros_like(q))
            gm = jnp.where(mine, g, jnp.zeros_like(g))
            inner = jnp.sum(jnp.where(mine, go, 0.0), axis=1, keepdims=True)
            ext = in_lanes(ln, three(jnp.broadcast_to(inner, (TILE, 128))))
            p = jnp.exp(nt(kc[...], jnp.concatenate([qm, l_ref[h]], axis=1)))
            dp = nt(vc[...], jnp.concatenate([gm, ext], axis=1))
            ds = (p * dp).astype(bf)
            dq = dq + tn(ds, km[h])
            probs.append(p.astype(bf))
            scores.append(ds)
            qs.append(qm)
            gs.append(gm)
        dva[...] += nn(probs[0], gs[0]) + nn(probs[1], gs[1])
        dka[...] += nn(scores[0], qs[0]) + nn(scores[1], qs[1])
        dq_ref[...] = (dq * 0.125).astype(bf)

        @pl.when(tile == tiles - 1)
        def _():
            dk_ref[...] = dka[...].astype(bf)
            dv_ref[...] = dva[...].astype(bf)

        at_steps(here, ends)

    tile_spec = pl.BlockSpec((TILE, 128), lambda p, i: (i, p))
    all_spec = pl.BlockSpec((n, 128), lambda p, i: (0, p))
    shapes = [jax.ShapeDtypeStruct(twos(high) + a.shape[len(bits) :], bf) for a in parts[: len(ahead)]]
    shapes += [jax.ShapeDtypeStruct(a.shape[len(bits) :], f32) for a in parts[len(ahead) :]]
    out = pl.pallas_call(
        kernel,
        grid=(pairs, tiles),
        out_shape=tuple(jax.ShapeDtypeStruct((n, w), bf) for _ in range(3)) + tuple(shapes),
        in_specs=[tile_spec, all_spec, all_spec, ANY, tile_spec, pl.BlockSpec((2, TILE, 128), lambda p, i: (p, i, 0))]
        + [ANY] * na,
        out_specs=(tile_spec, all_spec, all_spec) + (VMEM,) * na,
        scratch_shapes=[
            pltpu.VMEM((n, 256), bf),
            pltpu.VMEM((n, 256), bf),
            pltpu.VMEM((2, n, 128), bf),
            pltpu.VMEM((n, 128), f32),
            pltpu.VMEM((n, 128), f32),
            pltpu.VMEM((pairs, 2, half, 128), bf),
            DMA((3, pairs)),
        ]
        + scratch,
        compiler_params=pltpu.CompilerParams(collective_id=2, **SIDE),
    )(q, k, v, g, wide, logs, *parts)
    return out[:3], out[3 : 3 + len(ahead)], out[3 + len(ahead) :]


epsilon = 1e-05
root_half = 0.7071067811865476


def pad_rows(x, to):
    return jnp.pad(x, ((0, to - x.shape[0]), (0, 0)))


def norm_parts(rows_in):
    center = rows_in - jnp.mean(rows_in, axis=-1, keepdims=True)
    scale = lax.rsqrt(jnp.mean(center * center, axis=-1, keepdims=True) + epsilon)
    return center * scale, scale


def norm_back(gy, gain, xhat, scale):
    gt = gy * gain
    return scale * (gt - jnp.mean(gt, axis=-1, keepdims=True) - xhat * jnp.mean(gt * xhat, axis=-1, keepdims=True))


def per_device(
    clips,
    frames,
    norm1_gain,
    norm1_shift,
    query_weight,
    query_bias,
    key_weight,
    value_weight,
    value_bias,
    out_weight,
    out_bias,
    norm2_gain,
    norm2_shift,
    hidden_weight,
    hidden_bias,
    output_weight,
    output_bias,
    out_grad,
):
    seq = lax.axis_index("seq")
    valid, width = frames.shape[1], frames.shape[2]
    half = -(-valid // 256) * 256
    cols = width // 2
    devices = 2 * clips
    vectors = (norm1_gain, norm1_shift, query_bias, value_bias, out_bias, norm2_gain, norm2_shift, hidden_bias, output_bias)
    sizes = [v.shape[0] for v in vectors]
    packed, at = 0, 0
    for vector, size in zip(vectors, sizes):
        packed = packed + jnp.pad(vector, (at, 1024 - at - size))
        at += size
    (w_query, w_key, w_value), small, ahead, both = first_gather(
        clips, [query_weight, key_weight, value_weight], packed.reshape(8, 128), [hidden_weight, output_weight], frames[0]
    )
    small = small.reshape(devices, 1024).astype(f32)
    unpacked, at = [], 0
    for size in sizes:
        unpacked.append(small[:, at : at + size].reshape(-1))
        at += size
    gain_one, shift_one, b_query, b_value, b_out, gain_two, shift_two, b_hidden, b_output = unpacked
    b_query = lax.dynamic_slice_in_dim(b_query, seq * cols, cols)
    b_value = lax.dynamic_slice_in_dim(b_value, seq * cols, cols)

    def pad_both(x):
        return jnp.pad(x, ((0, 0), (0, half - valid), (0, 0))).reshape(2 * half, -1)

    xhat_both, scale_both = norm_parts(both.astype(f32))
    normed = pad_both((xhat_both * gain_one + shift_one).astype(bf))
    query = (nn(normed, w_query) + b_query).astype(bf)
    key = nn(normed, w_key).astype(bf)
    value = (nn(normed, w_value) + b_value).astype(bf)
    attended, wide, logs, (w_hidden, w_output, w_out) = attn_fwd(
        clips, query, key, value, [out_weight], ahead, half, valid
    )

    own = pad_rows(frames[0], half).astype(f32)
    hidden_in = own + nn(attended, w_out) + b_out
    xhat_two, scale_two = norm_parts(hidden_in)
    normed_two = (xhat_two * gain_two + shift_two).astype(bf)
    pre_act = nn(normed_two, w_hidden) + b_hidden
    cdf = 0.5 * (1.0 + lax.erf(pre_act * root_half))
    acted = (pre_act * cdf).astype(bf)
    encoded = (hidden_in + nn(acted, w_output) + b_output).astype(bf)[:valid]

    grad_ff = pad_rows(out_grad[0], half)
    grad_out = grad_ff.astype(f32)
    grad_w_output = tn(acted, grad_ff)
    slope = cdf + pre_act * jnp.exp(-0.5 * pre_act * pre_act) * 0.3989422804014327
    grad_pre = (nt(grad_ff, w_output) * slope).astype(bf)
    grad_w_hidden = tn(normed_two, grad_pre)
    gy_two = nt(grad_pre, w_hidden)
    grad_hidden_in = grad_out + norm_back(gy_two, gain_two, xhat_two, scale_two)
    grad_branch = grad_hidden_in.astype(bf)
    grad_w_out = tn(attended, grad_branch)
    grad_attended = nt(grad_branch, w_out).astype(bf)

    (query_grad, key_grad, value_grad), ahead, (own_out,) = attn_bwd(
        clips,
        query,
        key,
        value,
        grad_attended,
        wide,
        logs,
        [grad_w_hidden.astype(bf), grad_w_output.astype(bf)],
        [grad_w_out.astype(bf)],
        half,
        valid,
    )
    grad_w_query = tn(normed, query_grad)
    grad_w_key = tn(normed, key_grad)
    grad_w_value = tn(normed, value_grad)
    gy_one = nt(query_grad, w_query) + nt(key_grad, w_key) + nt(value_grad, w_value)

    def sums(x):
        return jnp.sum(x.astype(f32), axis=0)

    def spread(x):
        return lax.dynamic_update_slice_in_dim(jnp.zeros((width,), f32), x, seq * cols, 0)

    vector_sums = (
        sums(gy_one * pad_both(xhat_both)),
        sums(gy_one),
        spread(sums(query_grad)),
        spread(sums(value_grad)),
        sums(grad_branch),
        sums(gy_two * xhat_two),
        sums(gy_two),
        sums(grad_pre),
        sums(grad_ff),
    )
    packed_sums = jnp.concatenate([v.reshape(devices, -1) for v in vector_sums], axis=1)
    packed_sums = jnp.pad(packed_sums, ((0, 0), (0, 1024 - packed_sums.shape[1]))).reshape(devices * 8, 128)
    (own_query, own_key, own_value), own_small, (own_hidden, own_output), gy_got = last_scatter(
        clips,
        [grad_w_query.astype(bf), grad_w_key.astype(bf), grad_w_value.astype(bf)],
        packed_sums,
        ahead,
        gy_one.astype(bf).reshape(2, half, width),
    )
    gy_mine = lax.dynamic_slice_in_dim(gy_one, seq * half, half) + gy_got.astype(f32)
    xhat_one, scale_one = norm_parts(own)
    frames_grad = (grad_hidden_in + norm_back(gy_mine, gain_one, xhat_one, scale_one)).astype(bf)[:valid]

    own_small = own_small.reshape(-1)
    owned, at = [], 0
    for size in sizes:
        owned.append(own_small[at : at + size])
        at += size
    return (
        encoded[None],
        frames_grad[None],
        owned[0],
        owned[1],
        own_query,
        owned[2],
        own_key,
        own_value,
        owned[3],
        own_out,
        owned[4],
        owned[5],
        owned[6],
        own_hidden,
        owned[7],
        own_output,
        owned[8],
    )


def solution(mesh):
    rows, vector, matrix = P("clip", "seq", None), P(("clip", "seq")), P(("clip", "seq"), None)
    placed = (
        rows,
        vector,
        vector,
        matrix,
        vector,
        matrix,
        matrix,
        vector,
        matrix,
        vector,
        vector,
        vector,
        matrix,
        vector,
        matrix,
        vector,
        rows,
    )
    weights = placed[1:-1]
    return jax.shard_map(
        functools.partial(per_device, mesh.shape["clip"]),
        mesh=mesh,
        in_specs=placed,
        out_specs=(rows, rows) + weights,
        check_vma=False,
    )
```

```python
import functools

import jax
import jax.numpy as jnp
from jax import lax
from jax.experimental import pallas as pl
from jax.experimental.pallas import tpu as pltpu
from jax.sharding import PartitionSpec as P

bf, f32 = jnp.bfloat16, jnp.float32
MESH = pl.DeviceIdType.MESH
SEQ = "seq"
ANY = pl.BlockSpec(memory_space=pl.ANY)
VMEM = pl.BlockSpec(memory_space=pltpu.VMEM)
DMA = pltpu.SemaphoreType.DMA
SIDE = dict(has_side_effects=True, vmem_limit_bytes=62 << 20)


class Place:
    def __init__(self, clips):
        self.count = clips.bit_length() - 1
        self.clip = lax.axis_index("clip")
        self.seq = lax.axis_index("seq")

    def mine(self, bit):
        if bit == SEQ:
            return self.seq
        return lax.rem(lax.div(self.clip, 1 << bit), 2)

    def partner(self, bit):
        if bit == SEQ:
            return {"clip": self.clip, "seq": 1 - self.seq}
        return {"clip": self.clip + (1 - 2 * self.mine(bit)) * (1 << bit), "seq": self.seq}

    def index(self, dims, free, flipped=None):
        return tuple(slice(None) if b in free else 1 - self.mine(b) if b == flipped else self.mine(b) for b in dims)

    def greet(self):
        barrier = pltpu.get_barrier_semaphore()
        bits = all_bits(self.count)
        for bit in bits:
            pl.semaphore_signal(barrier, inc=1, device_id=self.partner(bit), device_id_type=MESH)
        pl.semaphore_wait(barrier, len(bits))


def all_bits(count):
    return [*reversed(range(count)), SEQ]


def high_bits(count):
    return list(reversed(range(2, count)))


def twos(bits):
    return (2,) * len(bits)


def remote(src, dst, sems, partner):
    return pltpu.make_async_remote_copy(
        src_ref=src, dst_ref=dst, send_sem=sems[0], recv_sem=sems[1], device_id=partner, device_id_type=MESH
    )


class Gather:
    def __init__(self, place, src, out, dims, order, sems, lead=(), part=(), give=None):
        self.place, self.src, self.out, self.dims, self.lead, self.part = place, src, out, dims, tuple(lead), tuple(part)
        self.order, self.sems, self.give = list(order), sems, give
        self.start = () if give is None else (SEQ,)

    @staticmethod
    def semaphores(order):
        return DMA((2, 2 * len(order) + 4))

    def at(self, free, flipped=None):
        return self.out.at[self.lead + self.place.index(self.dims, free, flipped) + self.part]

    def copy(self, k, src, dst, bit):
        return remote(src, dst, (self.sems.at[0, k], self.sems.at[1, k]), self.place.partner(bit))

    def local(self):
        return pltpu.make_async_copy(self.src, self.at(()), self.sems.at[0, 0])

    def trade(self):
        return self.copy(1, self.give, self.at(()), SEQ)

    def step(self, k):
        held = self.at(self.start + tuple(self.order[:k]))
        return self.copy(2 * k + 2, self.src if k == 0 and self.give is None else held, held, self.order[k])

    def hand(self, k):
        if k == 0:
            at = self.at(self.start)
            return self.copy(2 * len(self.order) + 2, self.src if self.give is None else at, at, 0)
        at = self.at(self.start + tuple(self.order[: k - 1]), self.order[k - 1])
        return self.copy(2 * k + 1, at, at, 0)

    def events(self):
        n = len(self.order)

        def begin():
            self.local().start()
            if self.give is not None:
                self.trade().start()
            else:
                self.step(0).start()
                self.hand(0).start()

        def traded():
            self.local().wait()
            self.trade().wait()
            self.step(0).start()
            self.hand(0).start()

        def arrived(k):
            self.step(k).wait_recv()
            if k == 0 and self.give is None:
                self.local().wait()
            if k + 1 < n:
                self.step(k + 1).start()
            self.hand(k + 1).start()

        def finish():
            for k in range(n):
                self.step(k).wait_send()
            for k in range(n + 1):
                self.hand(k).wait()

        run = [begin] + ([traded] if self.give is not None else [])
        return run + [functools.partial(arrived, k) for k in range(n)] + [finish]


class Scatter:
    def __init__(self, place, parts, dims, order, acc, recv, sems, final):
        self.place, self.parts, self.dims, self.order = place, parts, list(dims), list(order)
        self.acc, self.recv, self.sems, self.final = acc, recv, sems, final

    @staticmethod
    def scratch(dims, order, shard, dtype):
        n = len(dims)
        bufs = [pltpu.VMEM((2,) * (n - 1) + shard, dtype)]
        bufs += [pltpu.VMEM((2,) * (n - 1 - k) + shard, dtype) for k in range(len(order))]
        return bufs + [DMA((2, len(order) + 1))]

    def free(self, k):
        return tuple(b for b in self.dims if b not in self.order[: k + 1])

    def step(self, k):
        p, bit = self.place, self.order[k]
        if k == 0:
            src = self.parts.at[p.index(self.dims, self.free(k), bit)]
        else:
            src = self.acc.at[p.index([b for b in self.dims if b != self.order[0]], self.free(k), bit)]
        return remote(src, self.recv[k], (self.sems.at[0, k], self.sems.at[1, k]), p.partner(bit))

    def local(self):
        src = self.parts.at[self.place.index(self.dims, self.free(0))]
        return pltpu.make_async_copy(src, self.acc, self.sems.at[0, len(self.order)])

    def combine(self, k):
        p, free = self.place, self.free(k)

        def one(i, carry):
            at = {b: lax.rem(lax.div(i, 1 << pos), 2) for pos, b in enumerate(reversed(free))}
            full = tuple(at[b] if b in at else p.mine(b) for b in self.dims if b != self.order[0])
            value = self.acc[full].astype(f32) + self.recv[k][tuple(at[b] for b in free)].astype(f32)
            if k == len(self.order) - 1:
                self.final(tuple(at[b] for b in free), value)
            else:
                self.acc[full] = value.astype(self.acc.dtype)
            return carry

        if free:
            lax.fori_loop(0, 1 << len(free), one, 0)
        else:
            one(0, 0)

    def events(self):
        n = len(self.order)

        def begin():
            self.step(0).start()
            self.local().start()

        def arrived(k):
            if k == 0:
                self.local().wait()
            self.step(k).wait_recv()
            self.combine(k)
            if k + 1 < n:
                self.step(k + 1).start()

        def finish():
            for k in range(n):
                self.step(k).wait_send()

        return [begin] + [functools.partial(arrived, k) for k in range(n)] + [finish]


class Everywhere:
    def __init__(self, place, bits, bufs, final):
        self.place, self.bits = place, bits
        self.held, self.send, self.recv, self.sems = bufs
        self.final = final

    @staticmethod
    def scratch(bits, shape):
        many = (len(bits),) + shape
        return [pltpu.VMEM(shape, f32), pltpu.VMEM(many, f32), pltpu.VMEM(many, f32), DMA((2, len(bits)))]

    def step(self, k):
        sems = (self.sems.at[0, k], self.sems.at[1, k])
        return remote(self.send.at[k], self.recv.at[k], sems, self.place.partner(self.bits[k]))

    def events(self):
        n = len(self.bits)

        def begin(k):
            self.send[k] = self.held[...]
            self.step(k).start()

        def arrived(k):
            self.step(k).wait()
            self.held[...] = self.send[k] + self.recv[k]
            if k + 1 < n:
                begin(k + 1)
            else:
                self.final(self.held[...])

        return [functools.partial(begin, 0)] + [functools.partial(arrived, k) for k in range(n)]


def at_steps(here, plan):
    for step in sorted({s for s, _ in plan}):

        @pl.when(here == step)
        def _(step=step):
            for s, event in plan:
                if s == step:
                    event()


NEG = -1e30
TILE = 256


def nt(a, b):
    return lax.dot_general(a, b, (((1,), (1,)), ((), ())), preferred_element_type=f32)


def nn(a, b):
    return lax.dot_general(a, b, (((1,), (0,)), ((), ())), preferred_element_type=f32)


def tn(a, b):
    return lax.dot_general(a, b, (((0,), (0,)), ((), ())), preferred_element_type=f32)


def lanes(shape):
    return lax.broadcasted_iota(jnp.int32, shape, 1)


def padding(shape, half, valid):
    return lax.rem(lax.broadcasted_iota(jnp.int32, shape, 0), half) >= valid


def in_lanes(ln, pieces):
    out = 0.0
    for i, piece in reversed(list(enumerate(pieces))):
        out = jnp.where(ln == i, piece, out)
    return out.astype(bf)


def three(x):
    high = x.astype(bf).astype(f32)
    mid = (x - high).astype(bf).astype(f32)
    return [-high, -mid, -(x - high - mid)]


def attn_fwd(clips, frames, vectors, qkv, w_hidden, w_output, w_out):
    valid, width = frames.shape
    half = -(-valid // TILE) * TILE
    n, w = 2 * half, width // 2
    pairs, tiles = w // 128, n // TILE
    count = clips.bit_length() - 1
    bits, high = all_bits(count), high_bits(count)
    own = qkv.shape[1]
    last = pairs * tiles - 1
    near, far = [*high, 1, SEQ], [*high, SEQ, 1]
    split_h, split_o = w_hidden.shape[1] // 2, w_output.shape[1] // 2
    all_rows, first_cols, last_cols = slice(None), slice(0, split_h), slice(split_h, None)
    big = [
        (0, (all_rows, first_cols), near),
        (0, (all_rows, last_cols), far),
        (1, (all_rows, slice(0, split_o)), near),
        (1, (all_rows, slice(split_o, None)), far),
        (2, (all_rows, all_rows), [1, *high, SEQ]),
    ]
    around = [*high, 1]

    def kernel(frames_ref, vec_ref, qkv_ref, *refs):
        shards, refs = refs[:3], refs[3:]
        att_out, wide_ref, l_ref, q_ref, k_ref, v_ref, nrm, vec_out, w_own, w_other = refs[:10]
        gathered, refs = refs[10:13], refs[13:]
        kc, vc, att, other, w_buf, att_sems, frame_sems = refs[:7]
        vec_bufs, sems = refs[7:11], refs[11:]
        pair, tile = pl.program_id(0), pl.program_id(1)
        here = pair * tiles + tile
        place = Place(clips)
        seq = place.seq

        def att_copies(p):
            cols = pl.ds(pl.multiple_of(seq * w + p * 128, 128), 128)
            piece = pl.ds(p * 128, 128)
            mine = att.at[pl.ds(pl.multiple_of(seq * half, half), half), piece]
            theirs = att.at[pl.ds(pl.multiple_of((1 - seq) * half, half), half), piece]
            keep = pltpu.make_async_copy(mine, att_out.at[:, cols], att_sems.at[0, p])
            give = remote(theirs, att_out.at[:, cols], (att_sems.at[1, p], att_sems.at[2, p]), place.partner(SEQ))
            return keep, give

        def start_att(p):
            for c in att_copies(p):
                c.start()

        def columns(of_seq, p, many=1):
            return qkv_ref.at[:, :, pl.ds(pl.multiple_of(of_seq * w + p * 128, 128), many * 128)]

        def trading(j, out, part, p, mine, many=1):
            keep, give = columns(mine, p, many), columns(1 - mine, p, many)
            return Gather(place, keep, out, bits, around, sems[j], (all_rows,), part, give).events()

        weights = [
            trading(p, w_buf, (all_rows, slice(p * 128, (p + 1) * 128)), p, seq) for p in range(pairs)
        ]
        theirs = trading(pairs, w_other, (), 0, 1 - seq, pairs)
        loads = [
            Gather(place, shards[i].at[part], gathered[i], bits, order, sems[pairs + 1 + j], (), part).events()
            for j, (i, part, order) in enumerate(big)
        ]

        def vec_final(value):
            vec_out[...] = value

        vec = Everywhere(place, [SEQ, *around, 0], vec_bufs, vec_final)
        give_frames = remote(frames_ref, other, (frame_sems.at[0], frame_sems.at[1]), place.partner(SEQ))

        def norm_rows(src, y):
            nrm[y, half - TILE :, :] = jnp.zeros((TILE, width), bf)
            for r in range(half // TILE):
                at = slice(r * TILE, min(valid, (r + 1) * TILE))
                x = src[at, :].astype(f32)
                center = x - jnp.mean(x, axis=1, keepdims=True)
                xhat = center * lax.rsqrt(jnp.mean(center * center, axis=1, keepdims=True) + epsilon)
                nrm[y, at, :] = (xhat * vec_out[0:1, :] + vec_out[1:2, :]).astype(bf)

        def project(p):
            cols = slice(p * 384, (p + 1) * 384)
            for b in range(clips):
                at = tuple((b >> bit) & 1 for bit in bits if bit != SEQ)
                for i in range(3):
                    piece = [w_buf[(i, *at, y, all_rows, slice(p * 128, (p + 1) * 128))].astype(f32) for y in range(2)]
                    col = p * 384 + i * 128
                    w_own[b * 2 * own : (b + 1) * 2 * own, col : col + 128] = jnp.concatenate(piece, axis=0).astype(bf)
            at = pl.ds(pl.multiple_of(seq * w + p * 128, 128), 128)
            for y in range(2):
                x = nn(nrm[y], w_own[:, cols])
                rows = slice(y * half, (y + 1) * half)
                q_ref[rows, :] = (x[:, :128] + vec_out[2:3, at]).astype(bf)
                k_ref[rows, :] = x[:, 128:256].astype(bf)
                v_ref[rows, :] = (x[:, 256:] + vec_out[3:4, at]).astype(bf)
            ln = lanes((n, 128))
            kk = k_ref[...]
            ext = in_lanes(ln, [jnp.where(padding((n, 128), half, valid), NEG, 0.0)])
            zero = jnp.zeros_like(kk)
            kc[0, :, :128] = jnp.where(ln < 64, kk, zero)
            kc[1, :, :128] = jnp.where(ln < 64, zero, kk)
            kc[0, :, 128:] = ext
            kc[1, :, 128:] = ext
            vc[:, :128] = v_ref[...]
            vc[:, 128:] = jnp.ones((n, 128), bf)

        @pl.when(here == 0)
        def _():
            place.greet()
            vec.held[...] = vec_ref[...]
            vec_events = vec.events()
            vec_events.pop(0)()
            for e in weights:
                e[0]()
            give_frames.start()
            theirs[0]()
            loads[4][0]()
            for i in range(len(around) + 1):
                for e in weights:
                    e[i + 1]()
                if vec_events:
                    vec_events.pop(0)()
                if i == len(high) - 1:
                    loads[0][0]()
                    loads[1][0]()
            for i in range(2):
                loads[i][1]()
            for i in range(2, 4):
                loads[i][0]()
            for e in vec_events:
                e()
            norm_rows(frames_ref, seq)
            loads[4][1]()
            for e in weights:
                e[-1]()
            give_frames.wait()
            norm_rows(other, 1 - seq)

        at_steps(here, [(p * tiles, functools.partial(project, p)) for p in range(pairs)])

        ln = lanes((TILE, 128))
        q = q_ref[pl.ds(pl.multiple_of(tile * TILE, TILE), TILE), :]
        qc = jnp.concatenate([q * jnp.asarray(0.125, bf), in_lanes(ln, [1.0])], axis=1)
        heads = []
        for h in range(2):
            s = nt(qc, kc[h])
            top = jnp.max(s, axis=1, keepdims=True)
            o = nn(jnp.exp(s - top).astype(bf), vc[...])
            total = o[:, 128:]
            heads.append(o[:, :128] / total)
            l_ref[h] = in_lanes(ln, three(top + jnp.log(total)) + [1.0])
        wide = jnp.where(ln < 64, heads[0], heads[1])
        wide_ref[...] = wide
        for p in range(pairs):

            @pl.when(pair == p)
            def _(p=p):
                att[pl.ds(pl.multiple_of(tile * TILE, TILE), TILE), p * 128 : (p + 1) * 128] = wide.astype(bf)

        ends = [((p + 1) * tiles - 1, functools.partial(start_att, p)) for p in range(pairs)]

        def add(program, first, steps):
            ends.extend((min(last, s), e) for s, e in zip(steps + [last] * len(program), program[first:]))

        later = [2 * k for k in range(len(high) - 1)]
        add(loads[4], 2, [3, 7])
        add(loads[0], 2, [*later, len(later) + 3, 10])
        add(loads[1], 2, [*later, len(later) + 3, 10])
        add(loads[2], 1, [2, *(6 + k for k in later), 14])
        add(loads[3], 1, [2, *(6 + k for k in later), 14])
        add(theirs, 1, [1, 8, 11, 15])
        ends.sort(key=lambda e: e[0])
        at_steps(here, ends)

        @pl.when(here == last)
        def _():
            for p in range(pairs):
                for c in att_copies(p):
                    c.wait()

    once = dict(pipeline_mode=pl.Buffered(1))

    def whole(shape):
        return pl.BlockSpec(shape, lambda p, i: (0,) * len(shape), **once)

    tile_spec = pl.BlockSpec((TILE, 128), lambda p, i: (i, p))
    all_spec = pl.BlockSpec((n, 128), lambda p, i: (0, p))
    like = jax.ShapeDtypeStruct
    ins = (frames, vectors, qkv, w_hidden, w_output, w_out)
    out = pl.pallas_call(
        kernel,
        grid=(pairs, tiles),
        out_shape=(
            like((half, width), bf),
            like((n, w), f32),
            like((2 * pairs, n, 128), bf),
            like((n, w), bf),
            like((n, w), bf),
            like((n, w), bf),
            like((2, half, width), bf),
            like(vectors.shape, f32),
            like((width, 3 * w), bf),
            like((3,) + twos(bits) + (own, w), bf),
            *(like(twos(bits) + a.shape, bf) for a in (w_hidden, w_output, w_out)),
        ),
        in_specs=[whole(a.shape) for a in ins],
        out_specs=(
            ANY,
            tile_spec,
            pl.BlockSpec((2, TILE, 128), lambda p, i: (p, i, 0)),
            all_spec,
            all_spec,
            all_spec,
            whole((2, half, width)),
            whole(vectors.shape),
            whole((width, 3 * w)),
            ANY,
            ANY,
            ANY,
            ANY,
        ),
        scratch_shapes=[
            pltpu.VMEM((2, n, 256), bf),
            pltpu.VMEM((n, 256), bf),
            pltpu.VMEM((n, w), bf),
            pltpu.VMEM((valid, width), bf),
            pltpu.VMEM((3,) + twos(bits) + (own, w), bf),
            DMA((3, pairs)),
            DMA((2,)),
            *Everywhere.scratch(bits, vectors.shape),
            *[Gather.semaphores(around)] * (pairs + 1),
            *[Gather.semaphores(order) for _, _, order in big],
        ],
        compiler_params=pltpu.CompilerParams(collective_id=1, **SIDE),
    )(*ins)
    flat = [o.reshape((-1, o.shape[-1])) for o in out[10:]]
    return out[:6], out[6].reshape((n, width)), out[7], out[8], out[9].reshape((3, width, w)), *flat


def attn_bwd(clips, acts, mats, sums, grads, valid):
    q, k, v, g, wide, logs, normed, frames, gain, grad_in = acts
    w_own, w_other = mats
    n, w = q.shape
    width = 2 * w
    half = n // 2
    pairs, tiles = w // 128, n // TILE
    count = clips.bit_length() - 1
    bits, high = all_bits(count), high_bits(count)
    low = list(reversed(high))
    block = [b for b in bits if b != SEQ]
    devices = 2 * clips
    parts = [a.reshape(twos(bits) + (a.shape[0] // devices, a.shape[1])) for a in grads]
    orders = [[0, 1, SEQ, *low], [0, *low, 1, SEQ], [0, SEQ, 1, *low]]
    own = width // devices
    last = pairs * tiles - 1
    scratch = []

    def take(*specs):
        scratch.extend(specs)
        return len(scratch) - len(specs), len(scratch)

    grad_at = [take(*Scatter.scratch(bits, o, a.shape[len(bits) :], bf)) for a, o in zip(parts, orders)]
    around = [0, 1, *low]
    pair_at = [
        take(
            pltpu.VMEM(twos(block) + (2 * own, 3 * 128), bf),
            pltpu.VMEM((2, own, 3 * 128), bf),
            pltpu.VMEM((own, 3 * 128), bf),
            DMA((2,)),
            *Scatter.scratch(block, around, (2 * own, 3 * 128), bf),
        )
        for _ in range(pairs)
    ]
    row_at = take(
        pltpu.VMEM(twos(block) + (2 * own, 128), f32),
        pltpu.VMEM((2, own, 128), f32),
        pltpu.VMEM((own, 128), f32),
        DMA((2,)),
        *Scatter.scratch(block, around, (2 * own, 128), f32),
    )
    vec_at = take(*Everywhere.scratch(bits, (16, width)))
    misc_at = take(
        pltpu.VMEM((n, 256), bf),
        pltpu.VMEM((n, 256), bf),
        pltpu.VMEM((2, n, 128), bf),
        pltpu.VMEM((n, 128), f32),
        pltpu.VMEM((n, 128), f32),
        pltpu.VMEM((pairs, 2, half, 128), bf),
        DMA((3, pairs)),
        pltpu.VMEM((pairs, 2, half, 3 * 128), bf),
        pltpu.VMEM((pairs, half, 3 * 128), bf),
        DMA((2, pairs)),
        pltpu.VMEM((half, width), f32),
        pltpu.VMEM((width, 128), f32),
    )

    def kernel(q_ref, k_ref, v_ref, o_ref, l_ref, g_in, normed_ref, frames_ref, gain_ref, in_ref, w_mine, w_theirs, *refs):
        sum_refs, refs = refs[: len(sums)], refs[len(sums) :]
        grad_refs, refs = refs[:3], refs[3:]
        x_out, q_out, k_out, v_out, row_out, vec_out = refs[:6]
        grad_outs, bufs = refs[6:9], refs[9:]
        kc, vc, km, dka, dva, g_all, g_sems, dx, dxr, dx_sems, gy, rows = bufs[slice(*misc_at)]
        pair, tile = pl.program_id(0), pl.program_id(1)
        here = pair * tiles + tile
        place = Place(clips)
        seq = place.seq

        def g_copy(p, kept):
            mine = pl.ds(pl.multiple_of(seq * w + p * 128, 128), 128)
            theirs = pl.ds(pl.multiple_of((1 - seq) * w + p * 128, 128), 128)
            if kept:
                return pltpu.make_async_copy(g_in.at[:, mine], g_all.at[p, seq], g_sems.at[0, p])
            return remote(g_in.at[:, theirs], g_all.at[p, seq], (g_sems.at[1, p], g_sems.at[2, p]), place.partner(SEQ))

        def start_g():
            for p in range(pairs):
                g_copy(p, True).start()
                g_copy(p, False).start()

        def keep_g(p):
            g_copy(p, True).wait()

        def wait_g(p):
            g_copy(p, False).wait()

        def dx_copy(p):
            return remote(dx.at[p, 1 - seq], dxr.at[p], (dx_sems.at[0, p], dx_sems.at[1, p]), place.partner(SEQ))

        def add_gy(value, p, mats):
            gy[...] += nt(value, mats)

        grad_programs = []
        for at, src, out, order in zip(grad_at, grad_refs, grad_outs, orders):
            mine = bufs[slice(*at)]

            def final(where, value, out=out):
                out[...] = value

            grad_programs.append(Scatter(place, src, bits, order, mine[0], mine[1:-1], mine[-1], final).events())

        pair_programs = []
        for p, at in enumerate(pair_at):
            src, ends, got, sems, *mine = bufs[slice(*at)]

            def final(where, value, ends=ends):
                ends[0] = value[:own].astype(bf)
                ends[1] = value[own:].astype(bf)

            def trade(ends=ends, got=got, sems=sems):
                return remote(ends.at[1 - seq], got, (sems.at[0], sems.at[1]), place.partner(SEQ))

            def close(p=p, ends=ends, got=got, trade=trade):
                trade().wait()
                mine, theirs = ends[seq].astype(f32), got[...].astype(f32)
                for i, out in enumerate((q_out, k_out, v_out)):
                    piece = slice(i * 128, (i + 1) * 128)
                    out[:, pl.ds(pl.multiple_of(seq * w + p * 128, 128), 128)] = mine[:, piece]
                    out[:, pl.ds(pl.multiple_of((1 - seq) * w + p * 128, 128), 128)] = theirs[:, piece]

            events = Scatter(place, src, block, around, mine[0], mine[1:-1], mine[-1], final).events()
            events.insert(-1, lambda trade=trade: trade().start())
            pair_programs.append(events + [close])

        row_src, row_ends, row_got, row_sems, *mine = bufs[slice(*row_at)]

        def row_final(where, value):
            row_ends[0] = value[:own]
            row_ends[1] = value[own:]

        def row_trade():
            return remote(row_ends.at[1 - seq], row_got, (row_sems.at[0], row_sems.at[1]), place.partner(SEQ))

        def row_close():
            row_trade().wait()
            row_out[...] = row_ends[seq] + row_got[...]

        row_program = Scatter(place, row_src, block, around, mine[0], mine[1:-1], mine[-1], row_final).events()
        row_program.insert(-1, lambda: row_trade().start())
        row_program.append(row_close)

        def vec_final(value):
            vec_out[...] = value

        vec = Everywhere(place, bits, bufs[slice(*vec_at)], vec_final)
        vec_events = vec.events()

        def vec_load():
            at = 8
            vec.held[...] = jnp.zeros((16, width), f32)
            for ref in sum_refs:
                for j in range(ref.shape[1] // width):
                    vec.held[at : at + 1, :] = ref[:, j * width : (j + 1) * width]
                    at += 1

        plan = [(0, place.greet), (0, start_g), (0, vec_load)]
        plan += [(0, grad_programs[j][0]) for j in (1, 0, 2)]
        plan += [(p * tiles, functools.partial(keep_g, p)) for p in range(pairs)]
        plan += [(p * tiles + tiles // 2, functools.partial(wait_g, p)) for p in range(pairs)]
        at_steps(here, plan)

        @pl.when(tile == 0)
        def _():
            ln = lanes((n, 128))
            kk = k_ref[...]
            ext = in_lanes(ln, [1.0, 1.0, 1.0, jnp.where(padding((n, 128), half, valid), NEG, 0.0)])
            zero = jnp.zeros_like(kk)
            kc[:, :128] = kk
            kc[:, 128:] = ext
            km[0] = jnp.where(ln < 64, kk, zero)
            km[1] = jnp.where(ln < 64, zero, kk)
            vc[:, :128] = v_ref[...]
            vc[:, 128:] = ext
            dka[...] = jnp.zeros_like(dka)
            dva[...] = jnp.zeros_like(dva)

        @pl.when(here == 0)
        def _():
            gy[...] = jnp.zeros_like(gy)
            rows[...] = jnp.zeros_like(rows)

        ln = lanes((TILE, 128))
        q = q_ref[...] * jnp.asarray(0.125, bf)
        per = half // TILE
        row_half, row_at_ = lax.rem(lax.div(tile, per) + seq, 2), pl.ds(pl.multiple_of(lax.rem(tile, per) * TILE, TILE), TILE)
        g = g_all[pair, row_half, row_at_, :]
        go = g.astype(f32) * o_ref[...]
        probs, scores, qs, gs = [], [], [], []
        dq = jnp.zeros((TILE, 128), f32)
        for h in range(2):
            mine = (ln < 64) if h == 0 else (ln >= 64)
            qm = jnp.where(mine, q, jnp.zeros_like(q))
            gm = jnp.where(mine, g, jnp.zeros_like(g))
            inner = jnp.sum(jnp.where(mine, go, 0.0), axis=1, keepdims=True)
            ext = in_lanes(ln, three(jnp.broadcast_to(inner, (TILE, 128))))
            p = jnp.exp(nt(kc[...], jnp.concatenate([qm, l_ref[h]], axis=1)))
            dp = nt(vc[...], jnp.concatenate([gm, ext], axis=1))
            ds = (p * dp).astype(bf)
            dq = dq + tn(ds, km[h])
            probs.append(p.astype(bf))
            scores.append(ds)
            qs.append(qm)
            gs.append(gm)
        dva[...] += nn(probs[0], gs[0]) + nn(probs[1], gs[1])
        dka[...] += nn(scores[0], qs[0]) + nn(scores[1], qs[1])
        dx[pair, row_half, row_at_, 0:128] = (dq * 0.125).astype(bf)

        @pl.when(tile == tiles - 1)
        def _():
            for y in range(2):
                dx[pair, y, :, 128:256] = dka[y * half : (y + 1) * half, :].astype(bf)
                dx[pair, y, :, 256:384] = dva[y * half : (y + 1) * half, :].astype(bf)

        def pair_done(p):
            dx_copy(p).start()
            both = jnp.concatenate([dx[p, 0], dx[p, 1]], axis=0)
            weight_grad = tn(normed_ref[...], both)
            src = bufs[slice(*pair_at[p])][0]
            for b in range(clips):
                at = tuple((b >> bit) & 1 for bit in block)
                src[at] = weight_grad[b * 2 * own : (b + 1) * 2 * own].astype(bf)
            pair_programs[p][0]()
            col = jnp.sum(both.astype(f32), axis=0, keepdims=True)
            mats_own = w_mine[:, p * 384 : (p + 1) * 384].astype(f32)
            first = jnp.sum(mats_own * weight_grad, axis=1, keepdims=True)
            second = jnp.sum(mats_own * col, axis=1, keepdims=True)
            lnw = lanes((width, 128))
            rows[...] += jnp.where(lnw == 0, first, jnp.where(lnw == 1, second, 0.0))
            cols = pl.ds(pl.multiple_of(seq * w + p * 128, 128), 128)
            vec.held[0:1, cols] = col[:, :128]
            vec.held[1:2, cols] = col[:, 256:]
            if p == pairs - 1:
                for b in range(clips):
                    at = tuple((b >> bit) & 1 for bit in block)
                    row_src[at] = rows[b * 2 * own : (b + 1) * 2 * own, :]
                row_program[0]()
                vec_events[0]()
            add_gy(dx[p, seq], p, w_mine[:, p * 384 : (p + 1) * 384])

        def received(p):
            dx_copy(p).wait()
            add_gy(dxr[p], p, jnp.concatenate([w_theirs[i, :, p * 128 : (p + 1) * 128] for i in range(3)], axis=1))

        def finish_rows():
            gain_row = gain_ref[...]
            for r in range(half // TILE):
                at = slice(r * TILE, (r + 1) * TILE)
                top = min(valid, (r + 1) * TILE)
                here_rows = slice(r * TILE, top)
                x = frames_ref[here_rows, :].astype(f32)
                center = x - jnp.mean(x, axis=1, keepdims=True)
                scale = lax.rsqrt(jnp.mean(center * center, axis=1, keepdims=True) + epsilon)
                xhat = center * scale
                gt = gy[at, :][: top - r * TILE] * gain_row
                back = gt - jnp.mean(gt, axis=1, keepdims=True) - xhat * jnp.mean(gt * xhat, axis=1, keepdims=True)
                x_out[here_rows, :] = (in_ref[here_rows, :] + scale * back).astype(bf)

        ends = [((p + 1) * tiles - 1, functools.partial(pair_done, p)) for p in range(pairs)]
        tail, late = [], []
        for p in range(pairs - 1):
            after = (p + 1) * tiles
            ends.append((after + 4, functools.partial(received, p)))
            mine = []
            for k, e in enumerate(pair_programs[p][1:]):
                step = after + (1, 6, 10, last)[min(k, 3)]
                if step < last:
                    ends.append((step, e))
                else:
                    mine.append(e)
            late.append(mine)
        whens = [[1, 9, 14, last, last], [0, 7, 16, last, last], [1, 5, 10, 16, last]]
        for program, when in zip(grad_programs, whens):
            waits = program[1:-1]
            for k, e in enumerate(waits):
                step = when[min(k, 4)]
                (tail if step == last else ends).append((step, e))
            tail.append((last, program[-1]))
        ends.sort(key=lambda e: e[0])
        at_steps(here, ends)

        @pl.when(here == last)
        def _():
            chains = [pair_programs[pairs - 1][1:], row_program[1:], vec_events[1:], *late]
            chains += [[e for s, e in tail if any(e is x for x in program)] for program in grad_programs]
            extra = [functools.partial(received, pairs - 1), finish_rows]
            for i in range(max(len(c) for c in chains)):
                for c in chains:
                    if i < len(c):
                        c[i]()
                if i >= 1 and extra:
                    extra.pop(0)()
            for e in extra:
                e()

    once = dict(pipeline_mode=pl.Buffered(1))

    def whole(a):
        return pl.BlockSpec(a.shape, lambda p, i: (0,) * a.ndim, **once)

    def turned(i):
        return lax.rem(i + (tiles // 2) * lax.axis_index("seq"), tiles)

    tile_spec = pl.BlockSpec((TILE, 128), lambda p, i: (turned(i), p))
    all_spec = pl.BlockSpec((n, 128), lambda p, i: (0, p))
    shapes = [((valid, width), bf)] + [((own, width), f32)] * 3 + [((own, 128), f32), ((16, width), f32)]
    shapes += [(a.shape[len(bits) :], f32) for a in parts]
    out = pl.pallas_call(
        kernel,
        grid=(pairs, tiles),
        out_shape=tuple(jax.ShapeDtypeStruct(*s) for s in shapes),
        in_specs=[tile_spec, all_spec, all_spec, tile_spec, pl.BlockSpec((2, TILE, 128), lambda p, i: (p, turned(i), 0)), ANY]
        + [whole(a) for a in (normed, frames, gain, grad_in, w_own, w_other, *sums)]
        + [ANY] * 3,
        out_specs=tuple(pl.BlockSpec(s, lambda p, i: (0,) * len(s), **once) for s, _ in shapes),
        scratch_shapes=scratch,
        compiler_params=pltpu.CompilerParams(collective_id=2, **SIDE),
    )(q, k, v, wide, logs, g, normed, frames, gain, grad_in, w_own, w_other, *sums, *parts)
    return out[0], out[1:4], out[4], out[5], out[6:]


epsilon = 1e-05
root_half = 0.7071067811865476


def pad_rows(x, to):
    return jnp.pad(x, ((0, to - x.shape[0]), (0, 0)))


def norm_parts(rows_in):
    center = rows_in - jnp.mean(rows_in, axis=-1, keepdims=True)
    scale = lax.rsqrt(jnp.mean(center * center, axis=-1, keepdims=True) + epsilon)
    return center * scale, scale


def norm_back(gy, gain, xhat, scale):
    gt = gy * gain
    return scale * (gt - jnp.mean(gt, axis=-1, keepdims=True) - xhat * jnp.mean(gt * xhat, axis=-1, keepdims=True))


def per_device(
    clips,
    frames,
    norm1_gain,
    norm1_shift,
    query_weight,
    query_bias,
    key_weight,
    value_weight,
    value_bias,
    out_weight,
    out_bias,
    norm2_gain,
    norm2_shift,
    hidden_weight,
    hidden_bias,
    output_weight,
    output_bias,
    out_grad,
):
    seq = lax.axis_index("seq")
    valid, width = frames.shape[1], frames.shape[2]
    half = -(-valid // 256) * 256
    devices = 2 * clips
    mine = lax.axis_index("clip") * 2 + seq
    vectors = (norm1_gain, norm1_shift, query_bias, value_bias, out_bias, norm2_gain, norm2_shift, output_bias)
    rows = width // devices
    placed = lax.dynamic_update_slice(jnp.zeros((8, width), f32), jnp.stack(vectors).astype(f32), (0, mine * rows))
    hidden_size = hidden_bias.shape[0]
    hidden_placed = lax.dynamic_update_slice(
        jnp.zeros((hidden_size * devices,), f32), hidden_bias.astype(f32), (mine * hidden_size,)
    )
    placed = jnp.concatenate([placed, hidden_placed.reshape(-1, width)], axis=0)
    placed = jnp.pad(placed, ((0, -placed.shape[0] % 8), (0, 0)))
    qkv = jnp.stack((query_weight, key_weight, value_weight))
    (attended, wide, logs, query, key, value), normed, vec, w_own, w_other, w_hidden, w_output, w_out = attn_fwd(
        clips, frames[0], placed, qkv, hidden_weight, output_weight, out_weight
    )
    gain_one, b_out, gain_two, shift_two, b_output = (vec[i : i + 1] for i in (0, 4, 5, 6, 7))
    b_hidden = vec[8 : 8 + hidden_size * devices // width].reshape(1, -1)

    own = pad_rows(frames[0], half).astype(f32)
    hidden_in = own + nn(attended, w_out) + b_out
    xhat_two, scale_two = norm_parts(hidden_in)
    normed_two = (xhat_two * gain_two + shift_two).astype(bf)
    pre_act = nn(normed_two, w_hidden) + b_hidden
    cdf = 0.5 * (1.0 + lax.erf(pre_act * root_half))
    acted = (pre_act * cdf).astype(bf)
    encoded = (hidden_in + nn(acted, w_output) + b_output).astype(bf)[:valid]

    grad_ff = pad_rows(out_grad[0], half)
    grad_out = grad_ff.astype(f32)
    grad_w_output = tn(acted, grad_ff)
    slope = cdf + pre_act * jnp.exp(-0.5 * pre_act * pre_act) * 0.3989422804014327
    grad_pre = (nt(grad_ff, w_output) * slope).astype(bf)
    grad_w_hidden = tn(normed_two, grad_pre)
    gy_two = nt(grad_pre, w_hidden)
    grad_hidden_in = grad_out + norm_back(gy_two, gain_two, xhat_two, scale_two)
    grad_branch = grad_hidden_in.astype(bf)
    grad_w_out = tn(attended, grad_branch)
    grad_attended = nt(grad_branch, w_out).astype(bf)

    def sums(x):
        return jnp.sum(x.astype(f32), axis=0, keepdims=True)

    frames_grad, (own_query, own_key, own_value), by_row, totals, (own_hidden, own_output, own_out) = attn_bwd(
        clips,
        (query, key, value, grad_attended, wide, logs, normed, frames[0], gain_one, grad_hidden_in),
        (w_own, w_other),
        (sums(grad_branch), sums(gy_two * xhat_two), sums(gy_two), sums(grad_ff), sums(grad_pre)),
        (grad_w_hidden.astype(bf), grad_w_output.astype(bf), grad_w_out.astype(bf)),
        valid,
    )

    owned = lax.dynamic_slice_in_dim(totals, mine * rows, rows, 1)
    hidden_totals = totals[12 : 12 + hidden_size * devices // width].reshape(-1)
    own_hidden_bias = lax.dynamic_slice_in_dim(hidden_totals, mine * hidden_size, hidden_size)
    shift_grad = by_row[:, 1]
    gain_grad = (by_row[:, 0] - norm1_shift.astype(f32) * shift_grad) / norm1_gain.astype(f32)
    return (
        encoded[None],
        frames_grad[None],
        gain_grad,
        shift_grad,
        own_query,
        owned[0],
        own_key,
        own_value,
        owned[1],
        own_out,
        owned[8],
        owned[9],
        owned[10],
        own_hidden,
        own_hidden_bias,
        own_output,
        owned[11],
    )


def solution(mesh):
    rows, vector, matrix = P("clip", "seq", None), P(("clip", "seq")), P(("clip", "seq"), None)
    placed = (
        rows,
        vector,
        vector,
        matrix,
        vector,
        matrix,
        matrix,
        vector,
        matrix,
        vector,
        vector,
        vector,
        matrix,
        vector,
        matrix,
        vector,
        rows,
    )
    weights = placed[1:-1]
    return jax.shard_map(
        functools.partial(per_device, mesh.shape["clip"]),
        mesh=mesh,
        in_specs=placed,
        out_specs=(rows, rows) + weights,
        check_vma=False,
    )
```
